32 devices in a mesh: dp: 8 (over z, x), head: 4 (over y, core).
Axes of the slice: x: 2, y: 2, z: 4, core: 2. Of those that a mesh axis runs over, the one named last changes fastest.
Arguments:
- residual: bfloat16 [32, 4096], P('dp', 'head'), may hold values from -6 to 6
- query: bfloat16 [32, 32, 128], P('dp', 'head'), may hold values from -4.5 to 4.5
- fresh_token_keys: bfloat16 [32, 8, 128], P('dp', 'head'), may hold values from -4.5 to 4.5
- value_new: bfloat16 [32, 8, 128], P('dp', 'head'), may hold values from -24 to 24
- key_cache: bfloat16 [32, 8, 2048, 128], P('dp', 'head'), may hold values from -6 to 6
- value_cache: bfloat16 [32, 8, 2048, 128], P('dp', 'head'), may hold values from -6 to 6
- lengths: int32 [32], P('dp'), may hold values from 1024 to 2048, as said below
- pages: int32 [32, 8, 64], P('dp', 'head'), may hold values from 0 to 127, as said below
- w_out: bfloat16 [4096, 4096], P('head', 'dp'), may hold values from -0.75 to 0.75
- norm_gain: float32 [4096], P('head'), may hold values from 0.5 to 1.5
- expert_ids: int32 [32, 2], P('dp'), may hold values from 0 to 7, all different within a row; in each aligned block of 4 rows (0 to 3, 4 to 7, ...) at most 2 rows name the same one
- gate_weights: float32 [32, 2], P('dp'), may hold values from 0.1 to 1
- w_in: bfloat16 [8, 2, 4096, 7168], P('dp', None, None, 'head'), may hold values from -0.09375 to 0.09375
- w_down: bfloat16 [8, 7168, 4096], P('dp', 'head'), may hold values from -0.0625 to 0.0625
Outputs:
- layer_out: bfloat16 [32, 4096], P('dp', 'head')
The draws below stay inside these ranges and needn't reach their ends.
Inputs may be any that keep to these rules, and one draw needn't show every extreme that they name: `lengths`: each request's length; some request has exactly 2048 and some exactly 1024. `pages`: for each request and key head, 64 distinct page numbers, all below ceil(length / 16), always including the page that holds the request's last cached token; in no fixed order. `expert_ids`: per token 2 distinct experts; among the 4 tokens of one dp index no expert is named more than 2 times.
All inputs are finite; a program needn't handle non-finite values.
Results may differ from the reference program's by a relative error of at most 0.012.
Values may be sent and summed in bfloat16 or wider, within the bound.
No kernel may reach another device: no remote copies, remote signals or barrier semaphores. Data moves between devices by JAX's collectives and lax.ppermute only.
A program may use at most 128 MiB of HBM per device.

```python
import math
import jax
import jax.numpy as jnp
import numpy as np
from jax import lax

D = 4096
HEADS = 32
KV_HEADS = 8
HD = 128
EXPERTS = 8
TOP = 2
FF = 7168
PAGE = 16
SEL = 64
B_DEV = 4
LEN = 2048
BATCH = 32
PAGES = 128
GROUP = 1
MOST = 2


def draw_query(key, part):
    shape = (BATCH, HEADS, HD)
    base = jax.random.truncated_normal(jax.random.fold_in(key, 1), -4.5, 4.5, shape, jnp.float32)
    return base.astype(jnp.bfloat16)


def draw_fresh_token_keys(key, part):
    shape = (BATCH, KV_HEADS, HD)
    base = 2.0 * jax.random.truncated_normal(jax.random.fold_in(key, 2), -2.25, 2.25, shape, jnp.float32)
    return base.astype(jnp.bfloat16)


def page_plan(key):
    plan_key = jax.random.fold_in(key, 11)
    length_key, end_key, shift_key, score_key = jax.random.split(plan_key, 4)
    lengths = jax.random.randint(length_key, (BATCH,), SEL * PAGE, LEN + 1, dtype=jnp.int32)
    first_end = jax.random.randint(end_key, (), 0, BATCH, dtype=jnp.int32)
    offset_scores = jax.random.randint(shift_key, (), 0, BATCH - 1, dtype=jnp.int32)
    second_end = (first_end + 1 + offset_scores) % BATCH
    lengths = lengths.at[first_end].set(LEN).at[second_end].set(SEL * PAGE)
    used_pages = (lengths + PAGE - 1) // PAGE
    page_num = jnp.arange(PAGES, dtype=jnp.int32)[None, None, :]
    scores = jax.random.randint(score_key, (BATCH, KV_HEADS, PAGES), 0, 1 << 20, dtype=jnp.int32) * PAGES + page_num
    scores = jnp.where(page_num == used_pages[:, None, None] - 1, 1 << 30, scores)
    scores = jnp.where(page_num >= used_pages[:, None, None], -1, scores)
    chosen = jax.lax.top_k(scores, SEL)[1].astype(jnp.int32)
    return (lengths, chosen)


def draw_lengths(key, part):
    return page_plan(key)[0]


def draw_pages(key, part):
    return page_plan(key)[1]


def steps_of(own_key, shape, cuts, low, top_value):
    gain, own = 1.0, jax.random.fold_in(own_key, 6)
    for dim, parts in cuts:
        steps = jnp.exp(jax.random.uniform(jax.random.fold_in(own, dim), (parts,), jnp.float32, low / len(cuts), top_value / len(cuts)))
        gain = gain * jnp.repeat(steps, shape[dim] // parts).reshape([-1 if axis == dim else 1 for axis in range(len(shape))])
    return gain


def deal_out(rng, own, number, rows, amount, top, reach, skew):
    sequence = jax.random.permutation(rng, amount)
    packed, usual = shares(amount, rows * top, reach, skew, True), shares(amount, rows * top, reach, skew, False)
    places = jnp.arange(amount)

    def named(sizes, offset_by):
        used = int((sizes > 0).sum())
        fixed = max(1, used // 4)
        passed = fixed + (places - fixed + offset_by * (used - fixed)) % max(1, amount - fixed)
        return jnp.zeros((amount,), jnp.int32).at[sequence[jnp.where(places < fixed, places, passed)]].set(jnp.asarray(sizes, jnp.int32))

    sizes = jnp.where(number % 4 == 0, named(packed, number // 4), named(usual, number - number // 4 - 1))
    mixed = jax.random.permutation(jax.random.fold_in(own, 3), amount)
    source_of, taker = mixed[0:amount // 2 * 2:2], mixed[1:amount // 2 * 2:2]
    margin = jnp.minimum(sizes[source_of] - 1, reach - sizes[taker]) // 2
    margin = jnp.where((source_of == sequence[0]) | (taker == sequence[0]) | (sizes[taker] == 0), 0, jnp.maximum(margin, 0))
    passed = jax.random.randint(jax.random.fold_in(own, 4), (amount // 2,), 0, 1 << 20) % (margin + 1)
    sizes = sizes.at[source_of].add(-passed).at[taker].add(passed)
    items = jnp.searchsorted(jnp.cumsum(sizes), jnp.arange(rows * top), side="right").astype(jnp.int32)
    listing = items.reshape(top, rows).T
    listing = listing[jax.random.permutation(jax.random.fold_in(own, 1), rows)]
    offset_by = jax.random.randint(jax.random.fold_in(own, 2), (rows, 1), 0, top)
    return jnp.take_along_axis(listing, (jnp.arange(top)[None, :] + offset_by) % top, axis=1)


def shares(count, total, reach, slope, full):
    weights = [(1 << 20) // math.isqrt(rank ** slope) + 1 for rank in range(1, count + 1)]
    largest = reach if full else min(reach, max(-(-total // count), total * weights[0] // sum(weights)))
    least = 1 if total - largest >= count - 1 else 0
    given, surplus = [largest] + [least] * (count - 1), total - largest - least * (count - 1)
    while surplus > 0:
        free = [i for i in range(1, count) if given[i] < largest] or [i for i in range(1, count) if given[i] < reach]
        whole, remaining = sum([weights[i] for i in free]), surplus
        for i in free:
            addition = min(reach - given[i], max(1, remaining * weights[i] // whole), surplus)
            given[i] = given[i] + addition
            surplus = surplus - addition
    return np.array(given)


def noise(key, shape, spread, bound, cuts=(), held_as=jnp.bfloat16):
    drawn = spread * jax.random.normal(key, shape, jnp.float32)
    if cuts:
        drawn = drawn * steps_of(key, shape, cuts, -0.22, 0.18)
    return jnp.clip(drawn, -bound, bound).astype(held_as)


def setup_inputs(seed: int = 0) -> dict:
    key_list = jax.random.split(jax.random.key(seed), 15)
    residual = noise(key_list[0], (BATCH, D), 1.0, 6.0, ((0, 8), (1, 4)))
    query = draw_query(jax.random.fold_in(key_list[14], 71), 0)
    fresh_token_keys = draw_fresh_token_keys(jax.random.fold_in(key_list[14], 71), 0)
    value_new = noise(key_list[3], (BATCH, KV_HEADS, HD), 4.0, 24.0, ((0, 8), (1, 4)))
    key_cache = noise(key_list[4], (BATCH, KV_HEADS, LEN, HD), 1.0, 6.0, ((0, 8), (1, 4)))
    value_cache = noise(key_list[5], (BATCH, KV_HEADS, LEN, HD), 1.0, 6.0, ((0, 8), (1, 4)))
    lengths = draw_lengths(jax.random.fold_in(key_list[14], 71), 0)
    pages = draw_pages(jax.random.fold_in(key_list[14], 71), 0)
    w_out = noise(key_list[8], (HEADS * HD, D), 64 ** -0.5, 0.75, ((0, 4), (1, 8)))
    norm_gain = jnp.clip(1.0 + 0.1 * jax.random.normal(key_list[9], (D,), jnp.float32), 0.5, 1.5)
    expert_ids_keys = jax.random.split(jax.random.fold_in(key_list[10], 1), BATCH // B_DEV)
    expert_ids_turns = jax.random.permutation(jax.random.fold_in(key_list[10], 3), BATCH // B_DEV)
    expert_ids = jax.vmap(lambda own, number: deal_out(jax.random.fold_in(key_list[10], 2), own, number, B_DEV, EXPERTS, TOP, MOST, 2))(expert_ids_keys, expert_ids_turns).reshape((BATCH, TOP))
    gate_weights = jnp.clip(0.1 + 0.9 * jax.random.uniform(key_list[11], (BATCH, TOP), jnp.float32) ** steps_of(key_list[11], (BATCH, TOP), ((0, 8),), -0.2, 0.2), 0.1, 1.0)
    w_in = noise(key_list[12], (EXPERTS * GROUP, 2, D, FF // GROUP), D ** -0.5, 0.09375, ((0, 8), (3, 4)))
    w_down = noise(key_list[13], (EXPERTS * GROUP, FF // GROUP, D), FF ** -0.5, 0.0625, ((0, 8), (1, 4)))
    return {"residual": residual, "query": query, "fresh_token_keys": fresh_token_keys, "value_new": value_new, "key_cache": key_cache, "value_cache": value_cache, "lengths": lengths, "pages": pages, "w_out": w_out, "norm_gain": norm_gain, "expert_ids": expert_ids, "gate_weights": gate_weights, "w_in": w_in, "w_down": w_down}


EPSILON = 1e-05

def attend(request):
    query, fresh_token_keys, value_new, key_cache, value_cache, length, page_list = request
    offsets = jnp.arange(PAGE, dtype=jnp.int32)
    positions = (page_list[:, :, None] * PAGE + offsets[None, None, :]).reshape(KV_HEADS, SEL * PAGE).astype(jnp.int32)
    sel_keys = jnp.take_along_axis(key_cache, positions[:, :, None], axis=1).astype(jnp.float32)
    sel_values = jnp.take_along_axis(value_cache, positions[:, :, None], axis=1).astype(jnp.float32)
    grouped_rows = query.reshape(KV_HEADS, HEADS // KV_HEADS, HD).astype(jnp.float32)
    score_scale = HD ** (-0.5)
    scores = jnp.einsum('kgd,ksd->kgs', grouped_rows, sel_keys) * score_scale
    own_score = jnp.einsum('kgd,kd->kg', grouped_rows, fresh_token_keys.astype(jnp.float32)) * score_scale
    in_range = (positions < length)[:, None, :]
    masked = jnp.where(in_range, scores, -1e+30)
    row_top = jnp.maximum(lax.optimization_barrier(jnp.max(masked, axis=-1)), own_score)
    expo = jnp.where(in_range, jnp.exp(scores - row_top[..., None]), 0.0)
    own_expo = jnp.exp(own_score - row_top)
    denominator = lax.optimization_barrier(jnp.sum(expo, axis=-1)) + own_expo
    weights = (expo / denominator[..., None]).astype(jnp.bfloat16)
    own_weight = (own_expo / denominator).astype(jnp.bfloat16)
    attended = jnp.einsum('kgs,ksd->kgd', weights.astype(jnp.float32), sel_values)
    attended = attended + own_weight.astype(jnp.float32)[..., None] * value_new.astype(jnp.float32)[:, None, :]
    return attended.reshape(HEADS * HD).astype(jnp.bfloat16)

def reference(residual, query, fresh_token_keys, value_new, key_cache, value_cache, lengths, pages, w_out, norm_gain, expert_ids, gate_weights, w_in, w_down):
    attn_rows = lax.map(attend, (query, fresh_token_keys, value_new, key_cache, value_cache, lengths, pages))
    stream = residual.astype(jnp.float32) + jnp.dot(attn_rows, w_out, preferred_element_type=jnp.float32)
    square_mean_value = lax.optimization_barrier(jnp.mean(stream * stream, axis=-1))
    normed = (stream * lax.rsqrt(square_mean_value + EPSILON)[:, None] * norm_gain[None, :]).astype(jnp.bfloat16)
    expert_range = jnp.arange(EXPERTS, dtype=jnp.int32)
    weight_factor = lax.optimization_barrier(jnp.sum(jnp.where(expert_ids[:, :, None] == expert_range[None, None, :], gate_weights[:, :, None], 0.0), axis=1))

    def add_expert(carry, expert):
        expert_out = jnp.zeros((BATCH, D), jnp.float32)
        for slab_part in range(GROUP):
            slab = (expert * GROUP + slab_part).astype(jnp.int32)
            pair = lax.dynamic_index_in_dim(w_in, slab, 0, keepdims=False)
            gate_act = jnp.dot(normed, pair[0], preferred_element_type=jnp.float32)
            up_act = jnp.dot(normed, pair[1], preferred_element_type=jnp.float32)
            hidden = (jax.nn.silu(gate_act) * up_act).astype(jnp.bfloat16)
            down = lax.dynamic_index_in_dim(w_down, slab, 0, keepdims=False)
            expert_out = expert_out + jnp.dot(hidden, down, preferred_element_type=jnp.float32)
        column = lax.dynamic_index_in_dim(weight_factor, expert, 1, keepdims=False)
        return (carry + column[:, None] * expert_out, None)
    mixture, unused = lax.scan(add_expert, jnp.zeros((BATCH, D), jnp.float32), expert_range)
    return (stream + mixture).astype(jnp.bfloat16)
```

```python
import jax
import jax.numpy as jnp
from jax import lax
from jax.sharding import PartitionSpec as P

EXPERTS = 8
TOP = 2
PAGE = 16
MOST = 2
LANES = 128
BOTH = ("dp", "head")

EPSILON = 1e-05


def split3(x):
    high = lax.reduce_precision(x, 8, 7)
    mid = lax.reduce_precision(x - high, 8, 7)
    return tuple(part.astype(jnp.bfloat16) for part in (high, mid, x - high - mid))


def attend(query, fresh_token_keys, value_new, key_cache, value_cache, lengths, pages):
    tok_rows, head_local, head_dim = query.shape
    kv_local, cache_len = key_cache.shape[1:3]
    page_total = cache_len // PAGE
    group_member_count = head_local // kv_local
    page_numbers = jnp.arange(page_total, dtype=jnp.int32)
    page_chosen = jnp.any(pages[:, :, :, None] == page_numbers[None, None, None, :], axis=2)
    position_chosen = jnp.broadcast_to(
        page_chosen[:, :, :, None], (tok_rows, kv_local, page_total, PAGE)
    ).reshape(tok_rows, kv_local, cache_len)
    position_ids = jnp.arange(cache_len, dtype=jnp.int32)
    in_range = (position_chosen & (position_ids[None, None, :] < lengths[:, None, None]))[
        :, :, None, :
    ]
    grouped_rows = query.reshape(tok_rows, kv_local, group_member_count, head_dim)
    score_scale = head_dim ** (-0.5)
    scores = (
        jnp.einsum("bkgd,bksd->bkgs", grouped_rows, key_cache, preferred_element_type=jnp.float32)
        * score_scale
    )
    own_score = (
        jnp.einsum(
            "luxe,lue->lux", grouped_rows, fresh_token_keys, preferred_element_type=jnp.float32
        )
        * score_scale
    )
    masked = jnp.where(in_range, scores, -1e30)
    row_top = jnp.maximum(jnp.max(masked, axis=-1), own_score)
    expo = jnp.where(in_range, jnp.exp(scores - row_top[..., None]), 0.0)
    own_expo = jnp.exp(own_score - row_top)
    denominator = jnp.sum(expo, axis=-1) + own_expo
    weights = (expo / denominator[..., None]).astype(jnp.bfloat16)
    own_weight = (own_expo / denominator).astype(jnp.bfloat16)
    attended = jnp.einsum(
        "bkgs,bksd->bkgd", weights, value_cache, preferred_element_type=jnp.float32
    )
    attended = (
        attended
        + own_weight.astype(jnp.float32)[..., None] * value_new.astype(jnp.float32)[:, :, None, :]
    )
    return attended.reshape(tok_rows, head_local * head_dim).astype(jnp.bfloat16)


def slots_of(ids):
    owners, tok_rows, top = ids.shape
    flat = ids.reshape(owners, tok_rows * top)
    onehot = (flat[:, :, None] == jnp.arange(EXPERTS, dtype=jnp.int32)).astype(jnp.int32)
    same = (flat[:, :, None] == flat[:, None, :]).astype(jnp.int32)
    before = jnp.arange(tok_rows * top)[None, :] < jnp.arange(tok_rows * top)[:, None]
    place = jnp.sum(same * before[None].astype(jnp.int32), axis=2)
    taken = onehot[:, :, :, None] * (
        place[:, :, None, None] == jnp.arange(MOST, dtype=jnp.int32)
    ).astype(jnp.int32)
    return taken.reshape(owners, tok_rows, top, EXPERTS, MOST)


def shards(
    residual,
    query,
    fresh_token_keys,
    value_new,
    key_cache,
    value_cache,
    lengths,
    pages,
    w_out,
    norm_gain,
    expert_ids,
    gate_weights,
    w_in,
    w_down,
):
    dp_size, head_size = lax.axis_size("dp"), lax.axis_size("head")
    dp_at, head_at = lax.axis_index("dp"), lax.axis_index("head")
    group_count = dp_size // EXPERTS
    tok_rows = query.shape[0]
    batch = dp_size * tok_rows
    features = w_in.shape[2]
    col_width = w_out.shape[1]
    feat_width = residual.shape[1]
    ratio = feat_width // col_width
    half = col_width // 2
    head_rows = w_out.shape[0]

    attn_rows = attend(query, fresh_token_keys, value_new, key_cache, value_cache, lengths, pages)

    mine = (jnp.arange(head_size) == head_at)[:, None, None, None]
    residual_cut = residual.reshape(tok_rows, ratio, col_width).transpose(1, 0, 2)[None]
    residual_cut = jnp.where(mine, residual_cut, jnp.zeros((), jnp.bfloat16)).reshape(
        dp_size, tok_rows, col_width
    )
    routing = jnp.concatenate((expert_ids.astype(jnp.bfloat16),) + split3(gate_weights), axis=1)
    routing = jnp.pad(routing, ((0, 0), (0, LANES - routing.shape[1])))
    sent = jnp.concatenate(
        [
            jnp.broadcast_to(attn_rows, (dp_size,) + attn_rows.shape),
            residual_cut,
            jnp.broadcast_to(routing, (dp_size,) + routing.shape),
        ],
        axis=2,
    )
    came = lax.all_to_all(sent, "dp", split_axis=0, concat_axis=0, tiled=True)
    came = came.reshape(batch, came.shape[2])
    partial = jnp.dot(came[:, :head_rows], w_out, preferred_element_type=jnp.float32) + came[
        :, head_rows : head_rows + col_width
    ].astype(jnp.float32)
    routing = came[:, head_rows + col_width :]
    all_ids = routing[:, :TOP].astype(jnp.int32).reshape(dp_size, tok_rows, TOP)
    parts = routing[:, TOP : 4 * TOP].astype(jnp.float32).reshape(dp_size, tok_rows, 3, TOP)
    all_weights = parts[:, :, 0] + (parts[:, :, 1] + parts[:, :, 2])
    taken = slots_of(all_ids)

    gain_cut = lax.dynamic_index_in_dim(norm_gain.reshape(ratio, col_width), dp_at % ratio, 0)
    gain_cut = jnp.where(dp_at // ratio == head_at, gain_cut, 0.0)
    gain_high = lax.reduce_precision(gain_cut, 8, 7)
    partial = jnp.concatenate([partial, gain_high, gain_cut - gain_high], axis=0)
    core = head_at % 2
    kept = lax.dynamic_slice_in_dim(partial, core * half, half, axis=1)
    given = lax.dynamic_slice_in_dim(partial, (1 - core) * half, half, axis=1)
    swap = [(i, i ^ 1) for i in range(head_size)]
    chip_sum = kept + lax.ppermute(given.astype(jnp.bfloat16), "head", swap).astype(jnp.float32)
    chip_sum = chip_sum.astype(jnp.bfloat16)

    token_map = jnp.sum(taken, axis=2).astype(jnp.bfloat16)
    token_map = token_map.transpose(2, 0, 3, 1)
    own = jnp.eye(dp_size, dtype=jnp.bfloat16)
    picks = (token_map[:, :, :, None, :] * own[None, :, None, :, None]).reshape(
        EXPERTS * dp_size * MOST, batch
    )
    picked = jnp.dot(picks, chip_sum[:batch], preferred_element_type=jnp.float32)
    picked = picked.astype(jnp.bfloat16).reshape(EXPERTS, 1, 1, dp_size * MOST, half)
    gains = jnp.broadcast_to(chip_sum[batch:], (EXPERTS, 1, 1, 2, half))
    packet = jnp.concatenate([picked, gains], axis=3)
    packet = jnp.broadcast_to(
        packet, (EXPERTS, group_count, head_size) + packet.shape[3:]
    ).reshape((dp_size * head_size,) + packet.shape[3:])
    slot_rows = dp_size * MOST
    arrived = lax.all_to_all(packet, BOTH, split_axis=0, concat_axis=0, tiled=True)
    arrived = arrived.reshape(dp_size, head_size // 2, 2, slot_rows + 2, half)
    arrived = jnp.sum(arrived.astype(jnp.float32), axis=1)
    arrived = arrived.transpose(2, 0, 1, 3).reshape(slot_rows + 2, features)
    stream = arrived[:slot_rows]
    gain = arrived[slot_rows] + arrived[slot_rows + 1]
    square_mean = jnp.mean(stream * stream, axis=-1, keepdims=True)
    normed = (stream * lax.rsqrt(square_mean + EPSILON) * gain[None]).astype(jnp.bfloat16)

    gate_act = jnp.dot(normed, w_in[0, 0], preferred_element_type=jnp.float32)
    up_act = jnp.dot(normed, w_in[0, 1], preferred_element_type=jnp.float32)
    hidden = (jax.nn.silu(gate_act) * up_act).astype(jnp.bfloat16)
    slab_out = jnp.dot(hidden, w_down[0], preferred_element_type=jnp.float32)
    weighted = jnp.sum(taken.astype(jnp.float32) * all_weights[:, :, :, None, None], axis=(1, 2))
    slot_weights = lax.dynamic_index_in_dim(weighted, dp_at // group_count, 1, keepdims=False)
    slot_weights = slot_weights.reshape(slot_rows, 1)
    first = (head_at == 0) & (dp_at % group_count == 0)
    share = jnp.where(first, 1.0 / TOP, 0.0)
    given_back = (slot_weights * slab_out + share * stream).astype(jnp.bfloat16)

    given_back = given_back.reshape(dp_size, MOST, head_size, feat_width).transpose(0, 2, 1, 3)
    given_back = given_back.reshape(dp_size * head_size, MOST, feat_width)
    back = lax.all_to_all(given_back, BOTH, split_axis=0, concat_axis=0, tiled=True)
    own_map = jnp.sum(slots_of(expert_ids[None])[0], axis=1).astype(jnp.bfloat16)
    own_map = jnp.broadcast_to(
        own_map[:, :, None, None, :], (tok_rows, EXPERTS, group_count, head_size, MOST)
    ).reshape(tok_rows, dp_size * head_size * MOST)
    out = jnp.dot(
        own_map,
        back.reshape(dp_size * head_size * MOST, feat_width),
        preferred_element_type=jnp.float32,
    )
    return out.astype(jnp.bfloat16)


def solution(mesh):
    in_specs = (
        P("dp", "head"),
        P("dp", "head", None),
        P("dp", "head", None),
        P("dp", "head", None),
        P("dp", "head", None, None),
        P("dp", "head", None, None),
        P("dp"),
        P("dp", "head", None),
        P("head", "dp"),
        P("head"),
        P("dp", None),
        P("dp", None),
        P("dp", None, None, "head"),
        P("dp", "head", None),
    )
    out_specs = P("dp", "head")
    return jax.shard_map(shards, mesh=mesh, in_specs=in_specs, out_specs=out_specs, check_vma=False)
```

```python
import jax
import jax.numpy as jnp
from jax import lax
from jax.experimental import pallas as pl
from jax.experimental.pallas import tpu as pltpu
from jax.sharding import Mesh
from jax.sharding import PartitionSpec as P

EXPERTS = 8
TOP = 2
PAGE = 16
MOST = 2
LANES = 128
ROWS = 8
CORES = 2

EPSILON = 1e-05
MIB = 2**20
AHEAD = 4
EARLY = 3


def in_hbm(x):
    return pltpu.with_memory_space_constraint(x, pltpu.HBM)


def in_vmem(x):
    return pltpu.with_memory_space_constraint(x, pltpu.VMEM)


class Stream:
    def __init__(self, copies, ahead):
        self.copies, self.ahead, self.at = copies, ahead, 0
        for copy in copies[:ahead]:
            copy.start()

    def next(self):
        self.copies[self.at].wait()
        if self.at + self.ahead < len(self.copies):
            self.copies[self.at + self.ahead].start()
        self.at += 1


def by_head(parts, group):
    row = lax.broadcasted_iota(jnp.int32, parts[0].shape, 0)
    whole = parts[0]
    for k in range(1, len(parts)):
        whole = jnp.where(row >= k * group, parts[k], whole)
    return whole


def over_lanes(a, b):
    return lax.dot_general(a, b, (((1,), (1,)), ((), ())), preferred_element_type=jnp.float32)


def attend_kernel(
    lengths_at, query_at, fresh_at, value_at, pages_at, residual_at, ids_at, gates_at, keys_at,
    values_at, w_out_at, gain_at, out, w_out, gain, lengths, query, fresh, value, pages, residual,
    ids, gates, keys, values, scores, small_sems, sems,
):
    tok_rows, head_local, head_dim = query.shape
    kv_local, cache_len = keys.shape[1:3]
    group = head_local // kv_local
    page_total = cache_len // PAGE
    sel = pages.shape[2]
    pairs = (
        (lengths_at, lengths), (query_at, query), (fresh_at, fresh), (value_at, value),
        (pages_at, pages), (residual_at, residual), (ids_at, ids), (gates_at, gates),
    )
    small = [pltpu.make_async_copy(a, b, small_sems.at[i]) for i, (a, b) in enumerate(pairs)]
    pairs = [(keys_at.at[b], keys.at[b]) for b in range(tok_rows)]
    pairs += [(values_at.at[b], values.at[b]) for b in range(tok_rows)]
    pairs += [(w_out_at, w_out), (gain_at, gain)]
    for copy in small:
        copy.start()
    stream = Stream(
        [pltpu.make_async_copy(a, b, sems.at[i]) for i, (a, b) in enumerate(pairs)], AHEAD
    )

    page_of = lax.broadcasted_iota(jnp.int32, (page_total, cache_len), 1) // PAGE
    page = lax.broadcasted_iota(jnp.int32, (page_total, cache_len), 0)
    spread = jnp.where(page_of == page, 1.0, 0.0).astype(jnp.bfloat16)
    page = lax.broadcasted_iota(jnp.int32, (page_total, sel), 0)
    ones = jnp.ones((head_local, sel), jnp.bfloat16)
    position = lax.broadcasted_iota(jnp.int32, (head_local, cache_len), 1)
    scale = head_dim ** (-0.5)
    for copy in small:
        copy.wait()

    def beside(ref, b):
        return jnp.concatenate([ref[b, k] for k in range(kv_local)], axis=1)

    def apart(rows):
        row = lax.broadcasted_iota(jnp.int32, rows.shape, 0)
        wide_rows = rows.astype(jnp.float32)
        return jnp.concatenate(
            [jnp.where(row // group == k, wide_rows, 0.0) for k in range(kv_local)], axis=1
        ).astype(jnp.bfloat16)

    def wide(ref, b):
        each = ref[b].astype(jnp.float32)
        return by_head(
            [jnp.broadcast_to(each[k : k + 1], (head_local, head_dim)) for k in range(kv_local)],
            group,
        )

    chosen = []
    for b in range(tok_rows):
        named = pages[b]
        hits = [
            over_lanes(
                ones, jnp.where(page == named[k : k + 1], 1.0, 0.0).astype(jnp.bfloat16)
            )
            for k in range(kv_local)
        ]
        chosen.append(by_head(hits, group).astype(jnp.bfloat16))
    chosen = jnp.dot(
        jnp.concatenate(chosen, axis=0), spread, preferred_element_type=jnp.float32
    )
    for b in range(tok_rows):
        stream.next()
        live = (chosen[b * head_local : (b + 1) * head_local] > 0.5) & (
            position < lengths[0:1, b : b + 1]
        )
        raw = over_lanes(apart(query[b]), beside(keys, b))
        scores[b] = jnp.where(live, raw * scale, -1e30)
    weights, own_weights = [], []
    for b in range(tok_rows):
        score = scores[b]
        own = jnp.sum(query[b].astype(jnp.float32) * wide(fresh, b), axis=1, keepdims=True) * scale
        top = jnp.maximum(jnp.max(score, axis=1, keepdims=True), own)
        expo = jnp.exp(score - top)
        own_expo = jnp.exp(own - top)
        total = jnp.sum(expo, axis=1, keepdims=True) + own_expo
        weights.append((expo / total).astype(jnp.bfloat16))
        own_weights.append((own_expo / total).astype(jnp.bfloat16).astype(jnp.float32))
    done = []
    for b in range(tok_rows):
        stream.next()
        both = jnp.dot(weights[b], beside(values, b), preferred_element_type=jnp.float32)
        attended = by_head(
            [both[:, k * head_dim : (k + 1) * head_dim] for k in range(kv_local)], group
        )
        attended = attended + own_weights[b] * wide(value, b)
        done.append(
            jnp.concatenate([attended[r : r + 1] for r in range(head_local)], axis=1)
        )
    done = jnp.concatenate(done, axis=0).astype(jnp.bfloat16)

    dp_size = out.shape[0]
    rows_width = head_local * head_dim
    feat_width = residual.shape[1]
    col_width = out.shape[2] - rows_width - 2 * LANES
    ratio = feat_width // col_width
    dp_at = lax.axis_index("dp")
    head_at = lax.axis_index("y") * CORES + lax.axis_index("core")
    held = residual[...]

    def lanes_of(pair):
        pad = jnp.zeros((2 * TOP, LANES - tok_rows), jnp.float32)
        packed = jnp.concatenate([jnp.concatenate(pair, axis=0), pad], axis=1)
        return pltpu.roll(packed, dp_at * tok_rows, 1).astype(jnp.bfloat16)

    gate = gates[...]
    high = gate.astype(jnp.bfloat16).astype(jnp.float32)
    mid = (gate - high).astype(jnp.bfloat16).astype(jnp.float32)
    first = lanes_of([ids[...].astype(jnp.float32), high])
    second = lanes_of([mid, gate - high - mid])
    for to in range(dp_size):
        cut = held[:, (to % ratio) * col_width : (to % ratio + 1) * col_width]
        kept = jnp.where(head_at == to // ratio, cut.astype(jnp.float32), 0.0)
        out[to, :, 0:rows_width] = done
        out[to, :, rows_width : rows_width + col_width] = kept.astype(jnp.bfloat16)
        out[to, :, rows_width + col_width : rows_width + col_width + LANES] = first
        out[to, :, rows_width + col_width + LANES :] = second
    stream.next()
    stream.next()


def attend(args, dp_size):
    query, keys, w_out, norm_gain = args[1], args[8], args[10], args[11]
    col_width = w_out.shape[1]
    tok_rows, head_local, head_dim = query.shape
    cache_len = keys.shape[2]
    width = head_local * head_dim + col_width + 2 * LANES
    return pl.pallas_call(
        attend_kernel,
        out_shape=(
            jax.ShapeDtypeStruct((dp_size, tok_rows, width), jnp.bfloat16),
            pltpu.VMEM(w_out.shape, w_out.dtype),
            pltpu.VMEM(norm_gain.shape, norm_gain.dtype),
        ),
        in_specs=[pl.BlockSpec(memory_space=pl.ANY)] * len(args),
        out_specs=(pl.BlockSpec(memory_space=pltpu.VMEM),) * 3,
        scratch_shapes=[pltpu.VMEM(a.shape, a.dtype) for a in args[:10]]
        + [
            pltpu.VMEM((tok_rows, head_local, cache_len), jnp.float32),
            pltpu.SemaphoreType.DMA((8,)),
            pltpu.SemaphoreType.DMA((2 * tok_rows + 2,)),
        ],
        compiler_params=pltpu.CompilerParams(vmem_limit_bytes=58 * MIB),
        cost_estimate=pl.CostEstimate(
            flops=4 * tok_rows * head_local * cache_len * head_dim,
            bytes_accessed=4 * keys.size + 2 * w_out.size,
            transcendentals=tok_rows * head_local * cache_len,
        ),
        name="attend",
    )(*[in_hbm(a) for a in args])


def places_of(ids, tok_rows):
    lane = lax.broadcasted_iota(jnp.int32, (1, LANES), 1)
    places = []
    for j in range(TOP):
        place = jnp.zeros((1, LANES), jnp.int32)
        for back in range(1, tok_rows):
            same = jnp.zeros((1, LANES), jnp.bool_)
            for i in range(TOP):
                same = same | (ids[j] == pltpu.roll(ids[i], back, 1))
            place = place + jnp.where(same & (lane % tok_rows >= back), 1, 0)
        places.append(place)
    return places


def project_kernel(came, w_out, norm_gain, w_in, packet, factors, early, rows, sems):
    early_copy = pltpu.make_async_copy(
        w_in.at[0, 0, :, pl.ds(0, early.shape[1])], early, sems.at[0]
    )
    early_copy.start()
    dp_size, tok_rows, width = came.shape
    depth, col_width = w_out.shape
    batch = dp_size * tok_rows
    slot_rows = dp_size * MOST
    blocks = slot_rows // ROWS
    experts_at = depth + col_width
    ratio = norm_gain.shape[1] // col_width
    dp_at = lax.axis_index("dp")
    head_at = lax.axis_index("y") * CORES + lax.axis_index("core")
    group_count = dp_size // EXPERTS
    routing = jnp.zeros((tok_rows, 2 * LANES), jnp.float32)
    for d in range(dp_size):
        each = came[d].astype(jnp.float32)
        rows[d * tok_rows : (d + 1) * tok_rows] = each[:, :experts_at]
        routing = routing + each[:, experts_at:]
    ids = [routing[j : j + 1, :LANES].astype(jnp.int32) for j in range(TOP)]
    gates = [
        routing[TOP + j : TOP + j + 1, :LANES]
        + (routing[j : j + 1, LANES:] + routing[TOP + j : TOP + j + 1, LANES:])
        for j in range(TOP)
    ]
    lane = lax.broadcasted_iota(jnp.int32, (1, LANES), 1)
    places = places_of(ids, tok_rows)

    def takes(expert, place, owner):
        hits = []
        for j in range(TOP):
            hit = (owner == lane // tok_rows) & (expert == ids[j]) & (place == places[j])
            hits.append(hit)
        return hits

    row = lax.broadcasted_iota(jnp.int32, (EXPERTS * slot_rows, LANES), 0)
    hits = takes(row // slot_rows, row % MOST, row % slot_rows // MOST)
    picks = jnp.where(hits[0] | hits[1], 1.0, 0.0)[:, :batch].astype(jnp.bfloat16)
    partial = (
        jnp.dot(
            rows[:, :depth].astype(jnp.bfloat16), w_out[...], preferred_element_type=jnp.float32
        )
        + rows[:, depth:]
    ).astype(jnp.bfloat16)
    picked = jnp.dot(picks, partial, preferred_element_type=jnp.float32).astype(jnp.bfloat16)

    gain = jnp.zeros((1, col_width), jnp.float32)
    for r in range(ratio):
        gain = jnp.where(
            dp_at % ratio == r, norm_gain[:, r * col_width : (r + 1) * col_width], gain
        )
    gain = jnp.where(dp_at // ratio == head_at, gain, 0.0)
    high = gain.astype(jnp.bfloat16).astype(jnp.float32)
    gains = [
        part[:, i * LANES : (i + 1) * LANES]
        for part in (high, gain - high)
        for i in range(col_width // LANES)
    ]
    gains = gains + [jnp.zeros((1, LANES), jnp.float32)] * (ROWS - len(gains))
    gains = jnp.concatenate(gains, axis=0).astype(jnp.bfloat16)
    copies = packet.shape[0] // EXPERTS
    for e in range(EXPERTS):
        for i in range(copies):
            to = e * copies + i
            for k in range(blocks):
                first = e * slot_rows + k * ROWS
                packet[to, :, k * col_width : (k + 1) * col_width] = picked[first : first + ROWS]
            packet[to, :, blocks * col_width :] = gains

    row = lax.broadcasted_iota(jnp.int32, (slot_rows, LANES), 0)
    hits = takes(dp_at // group_count, row % MOST, row // MOST)
    weight = sum(jnp.where(hits[j], gates[j], 0.0) for j in range(TOP))
    factors[0] = jnp.broadcast_to(jnp.sum(weight, axis=1, keepdims=True), (slot_rows, LANES))
    first = (head_at == 0) & (dp_at % group_count == 0)
    factors[1] = jnp.full((slot_rows, LANES), jnp.where(first, 1.0 / TOP, 0.0))
    early_copy.wait()


def in_cut_of(w_in):
    return 2 * LANES if w_in.shape[3] % (2 * LANES) == 0 else w_in.shape[3]


def project(came, w_out, norm_gain, w_in, y_size):
    dp_size, tok_rows = came.shape[:2]
    depth, col_width = w_out.shape
    slot_rows = dp_size * MOST
    vmem, hbm = pl.BlockSpec(memory_space=pltpu.VMEM), pl.BlockSpec(memory_space=pl.ANY)
    return pl.pallas_call(
        project_kernel,
        out_shape=(
            jax.ShapeDtypeStruct(
                (dp_size * y_size, ROWS, slot_rows // ROWS * col_width + LANES), jnp.bfloat16
            ),
            jax.ShapeDtypeStruct((2, slot_rows, LANES), jnp.float32),
            pltpu.VMEM((w_in.shape[2], in_cut_of(w_in)), w_in.dtype),
        ),
        in_specs=[vmem, vmem, vmem, hbm],
        out_specs=(vmem, vmem, vmem),
        scratch_shapes=[
            pltpu.VMEM((dp_size * tok_rows, depth + col_width), jnp.float32),
            pltpu.SemaphoreType.DMA((1,)),
        ],
        compiler_params=pltpu.CompilerParams(vmem_limit_bytes=58 * MIB),
        cost_estimate=pl.CostEstimate(
            flops=2 * dp_size * tok_rows * depth * col_width,
            bytes_accessed=2 * depth * col_width,
            transcendentals=0,
        ),
        name="project",
    )(in_vmem(came), in_vmem(w_out), in_vmem(norm_gain), in_hbm(w_in))


def cut_at(w_in, at, in_cut):
    return w_in.at[0, at % 2, :, pl.ds(at // 2 * in_cut, in_cut)]


def early_kernel(arrived, w_in, early, sems):
    copies = [
        pltpu.make_async_copy(cut_at(w_in, 1 + i, early.shape[2]), early.at[i], sems.at[i])
        for i in range(early.shape[0])
    ]
    for copy in copies:
        copy.start()
    for copy in copies:
        copy.wait()


def load_early(arrived, w_in):
    count = min(EARLY, 2 * (w_in.shape[3] // in_cut_of(w_in))) - 1
    shape = (count, w_in.shape[2], in_cut_of(w_in))
    hbm = pl.BlockSpec(memory_space=pl.ANY)
    return pl.pallas_call(
        early_kernel,
        out_shape=pltpu.VMEM(shape, w_in.dtype),
        in_specs=[hbm, hbm],
        out_specs=pl.BlockSpec(memory_space=pltpu.VMEM),
        scratch_shapes=[pltpu.SemaphoreType.DMA((count,))],
        compiler_params=pltpu.CompilerParams(vmem_limit_bytes=1 * MIB),
        cost_estimate=pl.CostEstimate(
            flops=32 * shape[0] * shape[1] * shape[2],
            bytes_accessed=2 * shape[0] * shape[1] * shape[2],
            transcendentals=0,
        ),
        name="load_early",
    )(arrived, in_hbm(w_in))


def expert_kernel(
    arrived, swapped, factors, first_in, early_in, w_in, w_down, out, ins, downs, total, x,
    normed, hidden, in_sems, down_sems,
):
    slot_rows, features = x.shape
    in_cut = ins.shape[2]
    held = 1 + early_in.shape[0]
    in_count = hidden.shape[1] // in_cut
    down_count, down_cut = downs.shape[:2]
    copies = [
        pltpu.make_async_copy(cut_at(w_in, held + i, in_cut), ins.at[i], in_sems.at[i])
        for i in range(2 * in_count - held)
    ]
    copies += [
        pltpu.make_async_copy(
            w_down.at[0, pl.ds(j * down_cut, down_cut)], downs.at[j], down_sems.at[j]
        )
        for j in range(down_count)
    ]
    stream = Stream(copies, AHEAD)
    most, feat_width = out.shape[1:]
    heads = features // feat_width
    y_size = heads // CORES
    dp_size = arrived.shape[0] // y_size
    col_width = features // dp_size
    blocks = slot_rows // ROWS
    square = jnp.zeros((slot_rows, 1), jnp.float32)
    gain = []
    for d in range(dp_size):
        piece = jnp.zeros(arrived.shape[1:], jnp.float32)
        for y in range(y_size):
            at = d * y_size + y
            piece = piece + arrived[at].astype(jnp.float32)
            piece = piece + swapped[at].astype(jnp.float32)
        slots = jnp.concatenate(
            [piece[:, k * col_width : (k + 1) * col_width] for k in range(blocks)], axis=0
        )
        square = square + jnp.sum(slots * slots, axis=1, keepdims=True)
        x[:, d * col_width : (d + 1) * col_width] = slots
        terms = piece[:, blocks * col_width :]
        count = col_width // LANES
        for i in range(count):
            gain.append(terms[i : i + 1] + terms[count + i : count + i + 1])
    scale = lax.rsqrt(square * (1.0 / features) + EPSILON)
    for i in range(features // LANES):
        cut = slice(i * LANES, (i + 1) * LANES)
        normed[:, cut] = (x[:, cut] * scale * gain[i]).astype(jnp.bfloat16)
    for j in range(in_count):
        acts = []
        for i in range(2):
            at = 2 * j + i
            if at == 0:
                cut = first_in[...]
            elif at < held:
                cut = early_in[at - 1]
            else:
                stream.next()
                cut = ins[at - held]
            acts.append(jnp.dot(normed[...], cut, preferred_element_type=jnp.float32))
        hidden[:, j * in_cut : (j + 1) * in_cut] = (jax.nn.silu(acts[0]) * acts[1]).astype(
            jnp.bfloat16
        )
    weight, part = factors[0, :, 0:1], factors[1, :, 0:1]
    for j in range(down_count):
        stream.next()
        share = jnp.dot(
            hidden[:, j * down_cut : (j + 1) * down_cut],
            downs[j],
            preferred_element_type=jnp.float32,
        )
        total[...] = share if j == 0 else total[...] + share
    for h in range(heads):
        cut = slice(h * feat_width, (h + 1) * feat_width)
        given = weight * total[:, cut] + part * x[:, cut]
        for o in range(slot_rows // most):
            out[o * heads + h] = given[o * most : (o + 1) * most].astype(jnp.bfloat16)


def experts(arrived, swapped, factors, first_in, early_in, w_in, w_down, dp_size, feat_width):
    features, width = w_in.shape[2:]
    slot_rows = factors.shape[1]
    in_cut = in_cut_of(w_in)
    left = 2 * (width // in_cut) - 1 - early_in.shape[0]
    vmem, hbm = pl.BlockSpec(memory_space=pltpu.VMEM), pl.BlockSpec(memory_space=pl.ANY)
    return pl.pallas_call(
        expert_kernel,
        out_shape=jax.ShapeDtypeStruct(
            (dp_size * (features // feat_width), MOST, feat_width), jnp.bfloat16
        ),
        in_specs=[vmem] * 5 + [hbm] * 2,
        out_specs=vmem,
        scratch_shapes=[
            pltpu.VMEM((max(left, 1), features, in_cut), jnp.bfloat16),
            pltpu.VMEM((width // in_cut, in_cut, features), jnp.bfloat16),
            pltpu.VMEM((slot_rows, features), jnp.float32),
            pltpu.VMEM((slot_rows, features), jnp.float32),
            pltpu.VMEM((slot_rows, features), jnp.bfloat16),
            pltpu.VMEM((slot_rows, width), jnp.bfloat16),
            pltpu.SemaphoreType.DMA((max(left, 1),)),
            pltpu.SemaphoreType.DMA((width // in_cut,)),
        ],
        compiler_params=pltpu.CompilerParams(vmem_limit_bytes=48 * MIB),
        cost_estimate=pl.CostEstimate(
            flops=6 * slot_rows * features * width,
            bytes_accessed=6 * features * width,
            transcendentals=slot_rows * width,
        ),
        name="experts",
    )(
        in_vmem(arrived),
        in_vmem(swapped),
        in_vmem(factors),
        in_vmem(first_in),
        in_vmem(early_in),
        in_hbm(w_in),
        in_hbm(w_down),
    )


def combine_kernel(back, ids_at, out, rows):
    sources, most, feat_width = back.shape
    tok_rows = out.shape[0]
    pad = jnp.full((TOP, LANES - tok_rows), -1, jnp.int32)
    named = jnp.concatenate([ids_at[...], pad], axis=1)
    ids = [named[j : j + 1] for j in range(TOP)]
    places = places_of(ids, tok_rows)
    row = lax.broadcasted_iota(jnp.int32, (sources * most, LANES), 0)
    expert, place = row // (sources * most // EXPERTS), row % most
    takes = jnp.zeros(row.shape, jnp.float32)
    for j in range(TOP):
        takes = jnp.where((expert == ids[j]) & (place == places[j]), 1.0, takes)
    takes = jnp.transpose(takes)[:ROWS].astype(jnp.bfloat16)
    for i in range(sources):
        rows[i * most : (i + 1) * most] = back[i].astype(jnp.float32)
    total = jnp.dot(takes, rows[...].astype(jnp.bfloat16), preferred_element_type=jnp.float32)
    out[...] = total[:tok_rows].astype(jnp.bfloat16)


def combine(back, ids):
    sources, most, feat_width = back.shape
    tok_rows = ids.shape[1]
    vmem = pl.BlockSpec(memory_space=pltpu.VMEM)
    return pl.pallas_call(
        combine_kernel,
        out_shape=jax.ShapeDtypeStruct((tok_rows, feat_width), jnp.bfloat16),
        in_specs=[vmem, vmem],
        out_specs=vmem,
        scratch_shapes=[pltpu.VMEM((sources * most, feat_width), jnp.float32)],
        compiler_params=pltpu.CompilerParams(vmem_limit_bytes=16 * MIB),
        cost_estimate=pl.CostEstimate(
            flops=2 * tok_rows * back.size, bytes_accessed=2 * back.size, transcendentals=0
        ),
        name="combine",
    )(back, ids)


def shards(
    residual,
    query,
    fresh_token_keys,
    value_new,
    key_cache,
    value_cache,
    lengths,
    pages,
    w_out,
    norm_gain,
    expert_ids,
    gate_weights,
    w_in,
    w_down,
):
    dp_size, y_size = lax.axis_size("dp"), lax.axis_size("y")
    tok_rows, feat_width = residual.shape

    sent, w_out, norm_gain = attend(
        (
            lengths.reshape(1, tok_rows),
            query,
            fresh_token_keys,
            value_new,
            pages,
            residual,
            expert_ids.T,
            gate_weights.T,
            key_cache,
            value_cache,
            w_out,
            norm_gain.reshape(1, feat_width),
        ),
        dp_size,
    )
    came = lax.all_to_all(sent, "dp", split_axis=0, concat_axis=0, tiled=True)

    packet, factors, first_in = project(came, w_out, norm_gain, w_in, y_size)
    arrived = lax.all_to_all(packet, ("dp", "y"), split_axis=0, concat_axis=0, tiled=True)
    swapped = lax.ppermute(arrived, "core", [(i, i ^ 1) for i in range(CORES)])
    early_in = load_early(arrived, w_in)
    given_back = experts(
        arrived, swapped, factors, first_in, early_in, w_in, w_down, dp_size, feat_width
    )

    back = lax.all_to_all(
        given_back, ("dp", "y", "core"), split_axis=0, concat_axis=0, tiled=True
    )
    return combine(back, expert_ids.T)


def solution(mesh):
    dp_size, head_size = mesh.shape["dp"], mesh.shape["head"]
    grid = Mesh(mesh.devices.reshape(dp_size, head_size // CORES, CORES), ("dp", "y", "core"))
    head = ("y", "core")
    in_specs = (
        P("dp", head),
        P("dp", head, None),
        P("dp", head, None),
        P("dp", head, None),
        P("dp", head, None, None),
        P("dp", head, None, None),
        P("dp"),
        P("dp", head, None),
        P(head, "dp"),
        P(head),
        P("dp", None),
        P("dp", None),
        P("dp", None, None, head),
        P("dp", head, None),
    )
    return jax.shard_map(
        shards, mesh=grid, in_specs=in_specs, out_specs=P("dp", head), check_vma=False
    )
```

```python
import jax
import jax.numpy as jnp
from jax import lax
from jax.experimental import pallas as pl
from jax.experimental.pallas import tpu as pltpu
from jax.sharding import Mesh
from jax.sharding import PartitionSpec as P

EXPERTS = 8
TOP = 2
PAGE = 16
MOST = 2
LANES = 128
ROWS = 8
CORES = 2

EPSILON = 1e-05
MIB = 2**20
AHEAD = 4
EARLY = 3


def in_hbm(x):
    return pltpu.with_memory_space_constraint(x, pltpu.HBM)


def in_vmem(x):
    return pltpu.with_memory_space_constraint(x, pltpu.VMEM)


def in_cut_of(w_in):
    return 2 * LANES if w_in.shape[3] % (2 * LANES) == 0 else w_in.shape[3]


def cut_at(w_in, at, in_cut):
    return w_in.at[0, at % 2, :, pl.ds(at // 2 * in_cut, in_cut)]


class Stream:
    def __init__(self, copies, ahead):
        self.copies, self.ahead, self.at = copies, ahead, 0
        for copy in copies[:ahead]:
            copy.start()

    def next(self):
        self.copies[self.at].wait()
        if self.at + self.ahead < len(self.copies):
            self.copies[self.at + self.ahead].start()
        self.at += 1


def by_head(parts, group):
    row = lax.broadcasted_iota(jnp.int32, parts[0].shape, 0)
    whole = parts[0]
    for k in range(1, len(parts)):
        whole = jnp.where(row >= k * group, parts[k], whole)
    return whole


def over_lanes(a, b):
    return lax.dot_general(a, b, (((1,), (1,)), ((), ())), preferred_element_type=jnp.float32)


def attend_kernel(
    lengths_at, query_at, fresh_at, value_at, pages_at, residual_at, ids_at, gates_at, keys_at,
    values_at, w_out_at, gain_at, w_in, sent, w_out, gain, first_in, out, lengths, query, fresh, value, pages, residual,
    ids, gates, keys, values, scores, small_sems, sems,
):
    tok_rows, head_local, head_dim = query.shape
    kv_local, cache_len = keys.shape[1:3]
    group = head_local // kv_local
    page_total = cache_len // PAGE
    sel = pages.shape[2]
    pairs = (
        (lengths_at, lengths), (query_at, query), (fresh_at, fresh), (value_at, value),
        (pages_at, pages), (residual_at, residual), (ids_at, ids), (gates_at, gates),
    )
    small = [pltpu.make_async_copy(a, b, small_sems.at[i]) for i, (a, b) in enumerate(pairs)]
    span = tok_rows // (sems.shape[0] // 2 - 1)
    cuts = [pl.ds(b, span) for b in range(0, tok_rows, span)]
    pairs = [(keys_at.at[cut], keys.at[cut]) for cut in cuts]
    pairs += [(values_at.at[cut], values.at[cut]) for cut in cuts]
    pairs += [(w_out_at, w_out), (cut_at(w_in, 0, first_in.shape[1]), first_in)]
    small.append(pltpu.make_async_copy(gain_at, gain, small_sems.at[len(small)]))
    for copy in small:
        copy.start()
    stream = Stream(
        [pltpu.make_async_copy(a, b, sems.at[i]) for i, (a, b) in enumerate(pairs)], 3
    )

    page_of = lax.broadcasted_iota(jnp.int32, (page_total, cache_len), 1) // PAGE
    page = lax.broadcasted_iota(jnp.int32, (page_total, cache_len), 0)
    spread = jnp.where(page_of == page, 1.0, 0.0).astype(jnp.bfloat16)
    page = lax.broadcasted_iota(jnp.int32, (page_total, sel), 0)
    ones = jnp.ones((head_local, sel), jnp.bfloat16)
    position = lax.broadcasted_iota(jnp.int32, (head_local, cache_len), 1)
    scale = head_dim ** (-0.5)
    for copy in small:
        copy.wait()

    def beside(ref, b):
        return jnp.concatenate([ref[b, k] for k in range(kv_local)], axis=1)

    def apart(rows):
        row = lax.broadcasted_iota(jnp.int32, rows.shape, 0)
        wide_rows = rows.astype(jnp.float32)
        return jnp.concatenate(
            [jnp.where(row // group == k, wide_rows, 0.0) for k in range(kv_local)], axis=1
        ).astype(jnp.bfloat16)

    def wide(ref, b):
        each = ref[b].astype(jnp.float32)
        return by_head(
            [jnp.broadcast_to(each[k : k + 1], (head_local, head_dim)) for k in range(kv_local)],
            group,
        )

    chosen = []
    for b in range(tok_rows):
        named = pages[b]
        hits = [
            over_lanes(
                ones, jnp.where(page == named[k : k + 1], 1.0, 0.0).astype(jnp.bfloat16)
            )
            for k in range(kv_local)
        ]
        chosen.append(by_head(hits, group).astype(jnp.bfloat16))
    chosen = jnp.dot(
        jnp.concatenate(chosen, axis=0), spread, preferred_element_type=jnp.float32
    )
    for b in range(tok_rows):
        if b % span == 0:
            stream.next()
        live = (chosen[b * head_local : (b + 1) * head_local] > 0.5) & (
            position < lengths[0:1, b : b + 1]
        )
        raw = over_lanes(apart(query[b]), beside(keys, b))
        scores[b] = jnp.where(live, raw * scale, -1e30)
    weights, own_weights = [], []
    for b in range(tok_rows):
        score = scores[b]
        own = jnp.sum(query[b].astype(jnp.float32) * wide(fresh, b), axis=1, keepdims=True) * scale
        top = jnp.maximum(jnp.max(score, axis=1, keepdims=True), own)
        expo = jnp.exp(score - top)
        own_expo = jnp.exp(own - top)
        total = jnp.sum(expo, axis=1, keepdims=True) + own_expo
        weights.append((expo / total).astype(jnp.bfloat16))
        own_weights.append((own_expo / total).astype(jnp.bfloat16).astype(jnp.float32))
    done = []
    for b in range(tok_rows):
        if b % span == 0:
            stream.next()
        both = jnp.dot(weights[b], beside(values, b), preferred_element_type=jnp.float32)
        attended = by_head(
            [both[:, k * head_dim : (k + 1) * head_dim] for k in range(kv_local)], group
        )
        attended = attended + own_weights[b] * wide(value, b)
        done.append(
            jnp.concatenate([attended[r : r + 1] for r in range(head_local)], axis=1)
        )
    done = jnp.concatenate(done, axis=0).astype(jnp.bfloat16)

    dp_size = out.shape[0]
    rows_width = head_local * head_dim
    feat_width = residual.shape[1]
    col_width = out.shape[2] - rows_width - 2 * LANES
    ratio = feat_width // col_width
    dp_at = lax.axis_index("dp")
    head_at = lax.axis_index("y") * CORES + lax.axis_index("core")
    held = residual[...]

    def lanes_of(pair):
        pad = jnp.zeros((2 * TOP, LANES - tok_rows), jnp.float32)
        packed = jnp.concatenate([jnp.concatenate(pair, axis=0), pad], axis=1)
        return pltpu.roll(packed, dp_at * tok_rows, 1).astype(jnp.bfloat16)

    gate = gates[...]
    high = gate.astype(jnp.bfloat16).astype(jnp.float32)
    mid = (gate - high).astype(jnp.bfloat16).astype(jnp.float32)
    first = lanes_of([ids[...].astype(jnp.float32), high])
    second = lanes_of([mid, gate - high - mid])
    for to in range(dp_size):
        cut = held[:, (to % ratio) * col_width : (to % ratio + 1) * col_width]
        kept = jnp.where(head_at == to // ratio, cut.astype(jnp.float32), 0.0)
        out[to, :, 0:rows_width] = done
        out[to, :, rows_width : rows_width + col_width] = kept.astype(jnp.bfloat16)
        out[to, :, rows_width + col_width : rows_width + col_width + LANES] = first
        out[to, :, rows_width + col_width + LANES :] = second
    stream.next()
    packet_copy = pltpu.make_async_copy(out, sent, small_sems.at[len(small)])
    packet_copy.start()
    stream.next()
    packet_copy.wait()


def attend(args, dp_size):
    query, keys, w_out, norm_gain, w_in = args[1], args[8], args[10], args[11], args[12]
    col_width = w_out.shape[1]
    tok_rows, head_local, head_dim = query.shape
    cache_len = keys.shape[2]
    width = head_local * head_dim + col_width + 2 * LANES
    copies = 2 if tok_rows % 2 == 0 else tok_rows
    return pl.pallas_call(
        attend_kernel,
        out_shape=(
            pltpu.HBM((dp_size, tok_rows, width), jnp.bfloat16),
            pltpu.VMEM(w_out.shape, w_out.dtype),
            pltpu.VMEM(norm_gain.shape, norm_gain.dtype),
            pltpu.VMEM((w_in.shape[2], in_cut_of(w_in)), w_in.dtype),
        ),
        in_specs=[pl.BlockSpec(memory_space=pl.ANY)] * len(args),
        out_specs=(pl.BlockSpec(memory_space=pl.ANY),)
        + (pl.BlockSpec(memory_space=pltpu.VMEM),) * 3,
        scratch_shapes=[pltpu.VMEM((dp_size, tok_rows, width), jnp.bfloat16)]
        + [pltpu.VMEM(a.shape, a.dtype) for a in args[:10]]
        + [
            pltpu.VMEM((tok_rows, head_local, cache_len), jnp.float32),
            pltpu.SemaphoreType.DMA((10,)),
            pltpu.SemaphoreType.DMA((2 * copies + 2,)),
        ],
        compiler_params=pltpu.CompilerParams(vmem_limit_bytes=58 * MIB),
        cost_estimate=pl.CostEstimate(
            flops=4 * tok_rows * head_local * cache_len * head_dim,
            bytes_accessed=4 * keys.size + 2 * w_out.size,
            transcendentals=tok_rows * head_local * cache_len,
        ),
        name="attend",
    )(*[in_hbm(a) for a in args])


def places_of(ids, tok_rows):
    lane = lax.broadcasted_iota(jnp.int32, (1, LANES), 1)
    places = []
    for j in range(TOP):
        place = jnp.zeros((1, LANES), jnp.int32)
        for back in range(1, tok_rows):
            same = jnp.zeros((1, LANES), jnp.bool_)
            for i in range(TOP):
                same = same | (ids[j] == pltpu.roll(ids[i], back, 1))
            place = place + jnp.where(same & (lane % tok_rows >= back), 1, 0)
        places.append(place)
    return places


def project_kernel(came, w_out, norm_gain, packet, factors, rows):
    dp_size, tok_rows, width = came.shape
    depth, col_width = w_out.shape
    batch = dp_size * tok_rows
    slot_rows = dp_size * MOST
    blocks = slot_rows // ROWS
    experts_at = depth + col_width
    ratio = norm_gain.shape[1] // col_width
    dp_at = lax.axis_index("dp")
    head_at = lax.axis_index("y") * CORES + lax.axis_index("core")
    group_count = dp_size // EXPERTS
    routing = jnp.zeros((tok_rows, 2 * LANES), jnp.float32)
    for d in range(dp_size):
        each = came[d].astype(jnp.float32)
        rows[d * tok_rows : (d + 1) * tok_rows] = each[:, :experts_at]
        routing = routing + each[:, experts_at:]
    ids = [routing[j : j + 1, :LANES].astype(jnp.int32) for j in range(TOP)]
    gates = [
        routing[TOP + j : TOP + j + 1, :LANES]
        + (routing[j : j + 1, LANES:] + routing[TOP + j : TOP + j + 1, LANES:])
        for j in range(TOP)
    ]
    lane = lax.broadcasted_iota(jnp.int32, (1, LANES), 1)
    places = places_of(ids, tok_rows)

    def takes(expert, place, owner):
        hits = []
        for j in range(TOP):
            hit = (owner == lane // tok_rows) & (expert == ids[j]) & (place == places[j])
            hits.append(hit)
        return hits

    row = lax.broadcasted_iota(jnp.int32, (EXPERTS * slot_rows, LANES), 0)
    hits = takes(row // slot_rows, row % MOST, row % slot_rows // MOST)
    picks = jnp.where(hits[0] | hits[1], 1.0, 0.0)[:, :batch].astype(jnp.bfloat16)
    partial = (
        jnp.dot(
            rows[:, :depth].astype(jnp.bfloat16), w_out[...], preferred_element_type=jnp.float32
        )
        + rows[:, depth:]
    ).astype(jnp.bfloat16)
    picked = jnp.dot(picks, partial, preferred_element_type=jnp.float32).astype(jnp.bfloat16)

    gain = jnp.zeros((1, col_width), jnp.float32)
    for r in range(ratio):
        gain = jnp.where(
            dp_at % ratio == r, norm_gain[:, r * col_width : (r + 1) * col_width], gain
        )
    gain = jnp.where(dp_at // ratio == head_at, gain, 0.0)
    high = gain.astype(jnp.bfloat16).astype(jnp.float32)
    gains = [
        part[:, i * LANES : (i + 1) * LANES]
        for part in (high, gain - high)
        for i in range(col_width // LANES)
    ]
    gains = gains + [jnp.zeros((1, LANES), jnp.float32)] * (ROWS - len(gains))
    gains = jnp.concatenate(gains, axis=0).astype(jnp.bfloat16)
    copies = packet.shape[0] // EXPERTS
    for e in range(EXPERTS):
        for i in range(copies):
            to = e * copies + i
            for k in range(blocks):
                first = e * slot_rows + k * ROWS
                packet[to, :, k * col_width : (k + 1) * col_width] = picked[first : first + ROWS]
            packet[to, :, blocks * col_width :] = gains

    row = lax.broadcasted_iota(jnp.int32, (slot_rows, LANES), 0)
    hits = takes(dp_at // group_count, row % MOST, row // MOST)
    weight = sum(jnp.where(hits[j], gates[j], 0.0) for j in range(TOP))
    factors[0] = jnp.broadcast_to(jnp.sum(weight, axis=1, keepdims=True), (slot_rows, LANES))
    first = (head_at == 0) & (dp_at % group_count == 0)
    factors[1] = jnp.full((slot_rows, LANES), jnp.where(first, 1.0 / TOP, 0.0))


def project(came, w_out, norm_gain, y_size):
    dp_size, tok_rows = came.shape[:2]
    depth, col_width = w_out.shape
    slot_rows = dp_size * MOST
    vmem = pl.BlockSpec(memory_space=pltpu.VMEM)
    return pl.pallas_call(
        project_kernel,
        out_shape=(
            jax.ShapeDtypeStruct(
                (dp_size * y_size, ROWS, slot_rows // ROWS * col_width + LANES), jnp.bfloat16
            ),
            jax.ShapeDtypeStruct((2, slot_rows, LANES), jnp.float32),
        ),
        in_specs=[vmem] * 3,
        out_specs=(vmem, vmem),
        scratch_shapes=[pltpu.VMEM((dp_size * tok_rows, depth + col_width), jnp.float32)],
        compiler_params=pltpu.CompilerParams(vmem_limit_bytes=58 * MIB),
        cost_estimate=pl.CostEstimate(
            flops=2 * dp_size * tok_rows * depth * col_width,
            bytes_accessed=2 * depth * col_width,
            transcendentals=0,
        ),
        name="project",
    )(in_vmem(came), in_vmem(w_out), in_vmem(norm_gain))


def early_kernel(arrived, w_in, early, sems):
    copies = [
        pltpu.make_async_copy(cut_at(w_in, 1 + i, early.shape[2]), early.at[i], sems.at[i])
        for i in range(early.shape[0])
    ]
    for copy in copies:
        copy.start()
    for copy in copies:
        copy.wait()


def load_early(arrived, w_in):
    count = min(EARLY, 2 * (w_in.shape[3] // in_cut_of(w_in))) - 1
    shape = (count, w_in.shape[2], in_cut_of(w_in))
    hbm = pl.BlockSpec(memory_space=pl.ANY)
    return pl.pallas_call(
        early_kernel,
        out_shape=pltpu.VMEM(shape, w_in.dtype),
        in_specs=[hbm, hbm],
        out_specs=pl.BlockSpec(memory_space=pltpu.VMEM),
        scratch_shapes=[pltpu.SemaphoreType.DMA((count,))],
        compiler_params=pltpu.CompilerParams(vmem_limit_bytes=1 * MIB),
        cost_estimate=pl.CostEstimate(
            flops=32 * shape[0] * shape[1] * shape[2],
            bytes_accessed=2 * shape[0] * shape[1] * shape[2],
            transcendentals=0,
        ),
        name="load_early",
    )(arrived, in_hbm(w_in))


def expert_kernel(
    arrived, swapped, factors, first_in, early_in, w_in, w_down, out, ins, downs, total, x,
    normed, hidden, in_sems, down_sems,
):
    slot_rows, features = x.shape
    in_cut = ins.shape[2]
    held = 1 + early_in.shape[0]
    in_count = hidden.shape[1] // in_cut
    down_count, down_cut = downs.shape[:2]
    copies = [
        pltpu.make_async_copy(cut_at(w_in, held + i, in_cut), ins.at[i], in_sems.at[i])
        for i in range(2 * in_count - held)
    ]
    copies += [
        pltpu.make_async_copy(
            w_down.at[0, pl.ds(j * down_cut, down_cut)], downs.at[j], down_sems.at[j]
        )
        for j in range(down_count)
    ]
    stream = Stream(copies, AHEAD)
    most, feat_width = out.shape[1:]
    heads = features // feat_width
    y_size = heads // CORES
    dp_size = arrived.shape[0] // y_size
    col_width = features // dp_size
    blocks = slot_rows // ROWS
    square = jnp.zeros((slot_rows, 1), jnp.float32)
    gain = []
    for d in range(dp_size):
        piece = jnp.zeros(arrived.shape[1:], jnp.float32)
        for y in range(y_size):
            at = d * y_size + y
            piece = piece + arrived[at].astype(jnp.float32)
            piece = piece + swapped[at].astype(jnp.float32)
        slots = jnp.concatenate(
            [piece[:, k * col_width : (k + 1) * col_width] for k in range(blocks)], axis=0
        )
        square = square + jnp.sum(slots * slots, axis=1, keepdims=True)
        x[:, d * col_width : (d + 1) * col_width] = slots
        terms = piece[:, blocks * col_width :]
        count = col_width // LANES
        for i in range(count):
            gain.append(terms[i : i + 1] + terms[count + i : count + i + 1])
    scale = lax.rsqrt(square * (1.0 / features) + EPSILON)
    for i in range(features // LANES):
        cut = slice(i * LANES, (i + 1) * LANES)
        normed[:, cut] = (x[:, cut] * scale * gain[i]).astype(jnp.bfloat16)
    for j in range(in_count):
        acts = []
        for i in range(2):
            at = 2 * j + i
            if at == 0:
                cut = first_in[...]
            elif at < held:
                cut = early_in[at - 1]
            else:
                stream.next()
                cut = ins[at - held]
            acts.append(jnp.dot(normed[...], cut, preferred_element_type=jnp.float32))
        hidden[:, j * in_cut : (j + 1) * in_cut] = (jax.nn.silu(acts[0]) * acts[1]).astype(
            jnp.bfloat16
        )
    weight, part = factors[0, :, 0:1], factors[1, :, 0:1]
    last = down_count - 1
    if last == 0:
        total[...] = jnp.zeros_like(total)
    for j in range(last):
        stream.next()
        share = jnp.dot(
            hidden[:, j * down_cut : (j + 1) * down_cut],
            downs[j],
            preferred_element_type=jnp.float32,
        )
        total[...] = share if j == 0 else total[...] + share
    for h in range(heads):
        cut = slice(h * feat_width, (h + 1) * feat_width)
        if h == 0:
            stream.next()
        share = jnp.dot(
            hidden[:, last * down_cut :], downs[last, :, cut], preferred_element_type=jnp.float32
        )
        given = weight * (total[:, cut] + share) + part * x[:, cut]
        for o in range(slot_rows // most):
            out[o * heads + h] = given[o * most : (o + 1) * most].astype(jnp.bfloat16)


def experts(arrived, swapped, factors, first_in, early_in, w_in, w_down, dp_size, feat_width):
    features, width = w_in.shape[2:]
    slot_rows = factors.shape[1]
    in_cut = in_cut_of(w_in)
    left = 2 * (width // in_cut) - 1 - early_in.shape[0]
    vmem, hbm = pl.BlockSpec(memory_space=pltpu.VMEM), pl.BlockSpec(memory_space=pl.ANY)
    return pl.pallas_call(
        expert_kernel,
        out_shape=jax.ShapeDtypeStruct(
            (dp_size * (features // feat_width), MOST, feat_width), jnp.bfloat16
        ),
        in_specs=[vmem] * 5 + [hbm] * 2,
        out_specs=vmem,
        scratch_shapes=[
            pltpu.VMEM((max(left, 1), features, in_cut), jnp.bfloat16),
            pltpu.VMEM((width // in_cut, in_cut, features), jnp.bfloat16),
            pltpu.VMEM((slot_rows, features), jnp.float32),
            pltpu.VMEM((slot_rows, features), jnp.float32),
            pltpu.VMEM((slot_rows, features), jnp.bfloat16),
            pltpu.VMEM((slot_rows, width), jnp.bfloat16),
            pltpu.SemaphoreType.DMA((max(left, 1),)),
            pltpu.SemaphoreType.DMA((width // in_cut,)),
        ],
        compiler_params=pltpu.CompilerParams(vmem_limit_bytes=48 * MIB),
        cost_estimate=pl.CostEstimate(
            flops=6 * slot_rows * features * width,
            bytes_accessed=6 * features * width,
            transcendentals=slot_rows * width,
        ),
        name="experts",
    )(
        in_vmem(arrived),
        in_vmem(swapped),
        in_vmem(factors),
        in_vmem(first_in),
        in_vmem(early_in),
        in_hbm(w_in),
        in_hbm(w_down),
    )


def combine_kernel(back, ids_at, out, rows):
    sources, most, feat_width = back.shape
    tok_rows = out.shape[0]
    pad = jnp.full((TOP, LANES - tok_rows), -1, jnp.int32)
    named = jnp.concatenate([ids_at[...], pad], axis=1)
    ids = [named[j : j + 1] for j in range(TOP)]
    places = places_of(ids, tok_rows)
    row = lax.broadcasted_iota(jnp.int32, (sources * most, LANES), 0)
    expert, place = row // (sources * most // EXPERTS), row % most
    takes = jnp.zeros(row.shape, jnp.float32)
    for j in range(TOP):
        takes = jnp.where((expert == ids[j]) & (place == places[j]), 1.0, takes)
    takes = jnp.transpose(takes)[:ROWS].astype(jnp.bfloat16)
    for i in range(sources):
        rows[i * most : (i + 1) * most] = back[i].astype(jnp.float32)
    total = jnp.dot(takes, rows[...].astype(jnp.bfloat16), preferred_element_type=jnp.float32)
    out[...] = total[:tok_rows].astype(jnp.bfloat16)


def combine(back, ids):
    sources, most, feat_width = back.shape
    tok_rows = ids.shape[1]
    vmem = pl.BlockSpec(memory_space=pltpu.VMEM)
    return pl.pallas_call(
        combine_kernel,
        out_shape=jax.ShapeDtypeStruct((tok_rows, feat_width), jnp.bfloat16),
        in_specs=[vmem, vmem],
        out_specs=vmem,
        scratch_shapes=[pltpu.VMEM((sources * most, feat_width), jnp.float32)],
        compiler_params=pltpu.CompilerParams(vmem_limit_bytes=16 * MIB),
        cost_estimate=pl.CostEstimate(
            flops=2 * tok_rows * back.size, bytes_accessed=2 * back.size, transcendentals=0
        ),
        name="combine",
    )(back, ids)


def shards(
    residual,
    query,
    fresh_token_keys,
    value_new,
    key_cache,
    value_cache,
    lengths,
    pages,
    w_out,
    norm_gain,
    expert_ids,
    gate_weights,
    w_in,
    w_down,
):
    dp_size, y_size = lax.axis_size("dp"), lax.axis_size("y")
    tok_rows, feat_width = residual.shape

    sent, w_out, norm_gain, first_in = attend(
        (
            lengths.reshape(1, tok_rows),
            query,
            fresh_token_keys,
            value_new,
            pages,
            residual,
            expert_ids.T,
            gate_weights.T,
            key_cache,
            value_cache,
            w_out,
            norm_gain.reshape(1, feat_width),
            w_in,
        ),
        dp_size,
    )
    came = lax.all_to_all(sent, "dp", split_axis=0, concat_axis=0, tiled=True)

    packet, factors = project(came, w_out, norm_gain, y_size)
    arrived = lax.all_to_all(packet, ("dp", "y"), split_axis=0, concat_axis=0, tiled=True)
    swapped = lax.ppermute(arrived, "core", [(i, i ^ 1) for i in range(CORES)])
    early_in = load_early(arrived, w_in)
    given_back = experts(
        arrived, swapped, factors, first_in, early_in, w_in, w_down, dp_size, feat_width
    )

    back = lax.all_to_all(
        given_back, ("dp", "y", "core"), split_axis=0, concat_axis=0, tiled=True
    )
    return combine(back, expert_ids.T)


def solution(mesh):
    dp_size, head_size = mesh.shape["dp"], mesh.shape["head"]
    grid = Mesh(mesh.devices.reshape(dp_size, head_size // CORES, CORES), ("dp", "y", "core"))
    head = ("y", "core")
    in_specs = (
        P("dp", head),
        P("dp", head, None),
        P("dp", head, None),
        P("dp", head, None),
        P("dp", head, None, None),
        P("dp", head, None, None),
        P("dp"),
        P("dp", head, None),
        P(head, "dp"),
        P(head),
        P("dp", None),
        P("dp", None),
        P("dp", None, None, head),
        P("dp", head, None),
    )
    return jax.shard_map(
        shards, mesh=grid, in_specs=in_specs, out_specs=P("dp", head), check_vma=False
    )
```

```python
import jax
import jax.numpy as jnp
from jax import lax
from jax.experimental import pallas as pl
from jax.experimental.pallas import tpu as pltpu
from jax.sharding import Mesh
from jax.sharding import PartitionSpec as P

EXPERTS = 8
TOP = 2
PAGE = 16
MOST = 2
LANES = 128
ROWS = 8
CORES = 2

EPSILON = 1e-05
MIB = 2**20
AHEAD = 4
EARLY = 2


def in_hbm(x):
    return pltpu.with_memory_space_constraint(x, pltpu.HBM)


def in_vmem(x):
    return pltpu.with_memory_space_constraint(x, pltpu.VMEM)


def in_cut_of(w_in):
    return 2 * LANES if w_in.shape[3] % (2 * LANES) == 0 else w_in.shape[3]


def cut_at(w_in, at, in_cut):
    return w_in.at[0, at % 2, :, pl.ds(at // 2 * in_cut, in_cut)]


class Stream:
    def __init__(self, copies, ahead):
        self.copies, self.ahead, self.at = copies, ahead, 0
        for copy in copies[:ahead]:
            copy.start()

    def next(self):
        self.copies[self.at].wait()
        if self.at + self.ahead < len(self.copies):
            self.copies[self.at + self.ahead].start()
        self.at += 1


def by_head(parts, group):
    row = lax.broadcasted_iota(jnp.int32, parts[0].shape, 0)
    whole = parts[0]
    for k in range(1, len(parts)):
        whole = jnp.where(row >= k * group, parts[k], whole)
    return whole


def over_lanes(a, b):
    return lax.dot_general(a, b, (((1,), (1,)), ((), ())), preferred_element_type=jnp.float32)


def attend_kernel(
    lengths_at, query_at, fresh_at, value_at, pages_at, residual_at, ids_at, gates_at, keys_at,
    values_at, w_out_at, gain_at, w_in, sent, w_out, gain, first_in, out, lengths, query, fresh, value, pages, residual,
    ids, gates, keys, values, scores, small_sems, sems,
):
    tok_rows, head_local, head_dim = query.shape
    kv_local, cache_len = keys.shape[1:3]
    group = head_local // kv_local
    page_total = cache_len // PAGE
    sel = pages.shape[2]
    pairs = (
        (lengths_at, lengths), (query_at, query), (fresh_at, fresh), (value_at, value),
        (pages_at, pages), (residual_at, residual), (ids_at, ids), (gates_at, gates),
    )
    small = [pltpu.make_async_copy(a, b, small_sems.at[i]) for i, (a, b) in enumerate(pairs)]
    span = tok_rows // (sems.shape[0] // 2 - 1)
    cuts = [pl.ds(b, span) for b in range(0, tok_rows, span)]
    pairs = [(keys_at.at[cut], keys.at[cut]) for cut in cuts]
    pairs += [(values_at.at[cut], values.at[cut]) for cut in cuts]
    pairs += [(w_out_at, w_out), (cut_at(w_in, 0, first_in.shape[1]), first_in)]
    small.append(pltpu.make_async_copy(gain_at, gain, small_sems.at[len(small)]))
    for copy in small:
        copy.start()
    stream = Stream(
        [pltpu.make_async_copy(a, b, sems.at[i]) for i, (a, b) in enumerate(pairs)], 3
    )

    page_of = lax.broadcasted_iota(jnp.int32, (page_total, cache_len), 1) // PAGE
    page = lax.broadcasted_iota(jnp.int32, (page_total, cache_len), 0)
    spread = jnp.where(page_of == page, 1.0, 0.0).astype(jnp.bfloat16)
    page = lax.broadcasted_iota(jnp.int32, (page_total, sel), 0)
    ones = jnp.ones((head_local, sel), jnp.bfloat16)
    position = lax.broadcasted_iota(jnp.int32, (head_local, cache_len), 1)
    scale = head_dim ** (-0.5)
    for copy in small:
        copy.wait()

    def beside(ref, b):
        return jnp.concatenate([ref[b, k] for k in range(kv_local)], axis=1)

    def apart(rows):
        row = lax.broadcasted_iota(jnp.int32, rows.shape, 0)
        wide_rows = rows.astype(jnp.float32)
        return jnp.concatenate(
            [jnp.where(row // group == k, wide_rows, 0.0) for k in range(kv_local)], axis=1
        ).astype(jnp.bfloat16)

    def wide(ref, b):
        each = ref[b].astype(jnp.float32)
        return by_head(
            [jnp.broadcast_to(each[k : k + 1], (head_local, head_dim)) for k in range(kv_local)],
            group,
        )

    chosen = []
    for b in range(tok_rows):
        named = pages[b]
        hits = [
            over_lanes(
                ones, jnp.where(page == named[k : k + 1], 1.0, 0.0).astype(jnp.bfloat16)
            )
            for k in range(kv_local)
        ]
        chosen.append(by_head(hits, group).astype(jnp.bfloat16))
    chosen = jnp.dot(
        jnp.concatenate(chosen, axis=0), spread, preferred_element_type=jnp.float32
    )
    for b in range(tok_rows):
        if b % span == 0:
            stream.next()
        live = (chosen[b * head_local : (b + 1) * head_local] > 0.5) & (
            position < lengths[0:1, b : b + 1]
        )
        raw = over_lanes(apart(query[b]), beside(keys, b))
        scores[b] = jnp.where(live, raw * scale, -1e30)
    weights, own_weights = [], []
    for b in range(tok_rows):
        score = scores[b]
        own = jnp.sum(query[b].astype(jnp.float32) * wide(fresh, b), axis=1, keepdims=True) * scale
        top = jnp.maximum(jnp.max(score, axis=1, keepdims=True), own)
        expo = jnp.exp(score - top)
        own_expo = jnp.exp(own - top)
        total = jnp.sum(expo, axis=1, keepdims=True) + own_expo
        weights.append((expo / total).astype(jnp.bfloat16))
        own_weights.append((own_expo / total).astype(jnp.bfloat16).astype(jnp.float32))
    done = []
    for b in range(tok_rows):
        if b % span == 0:
            stream.next()
        both = jnp.dot(weights[b], beside(values, b), preferred_element_type=jnp.float32)
        attended = by_head(
            [both[:, k * head_dim : (k + 1) * head_dim] for k in range(kv_local)], group
        )
        attended = attended + own_weights[b] * wide(value, b)
        done.append(
            jnp.concatenate([attended[r : r + 1] for r in range(head_local)], axis=1)
        )
    done = jnp.concatenate(done, axis=0).astype(jnp.bfloat16)

    dp_size = out.shape[0]
    rows_width = head_local * head_dim
    feat_width = residual.shape[1]
    col_width = out.shape[2] - rows_width - 2 * LANES
    ratio = feat_width // col_width
    dp_at = lax.axis_index("dp")
    head_at = lax.axis_index("y") * CORES + lax.axis_index("core")
    held = residual[...]

    def lanes_of(pair):
        pad = jnp.zeros((2 * TOP, LANES - tok_rows), jnp.float32)
        packed = jnp.concatenate([jnp.concatenate(pair, axis=0), pad], axis=1)
        return pltpu.roll(packed, dp_at * tok_rows, 1).astype(jnp.bfloat16)

    gate = gates[...]
    high = gate.astype(jnp.bfloat16).astype(jnp.float32)
    mid = (gate - high).astype(jnp.bfloat16).astype(jnp.float32)
    first = lanes_of([ids[...].astype(jnp.float32), high])
    second = lanes_of([mid, gate - high - mid])
    for to in range(dp_size):
        cut = held[:, (to % ratio) * col_width : (to % ratio + 1) * col_width]
        kept = jnp.where(head_at == to // ratio, cut.astype(jnp.float32), 0.0)
        out[to, :, 0:rows_width] = done
        out[to, :, rows_width : rows_width + col_width] = kept.astype(jnp.bfloat16)
        out[to, :, rows_width + col_width : rows_width + col_width + LANES] = first
        out[to, :, rows_width + col_width + LANES :] = second
    stream.next()
    packet_copy = pltpu.make_async_copy(out, sent, small_sems.at[len(small)])
    packet_copy.start()
    stream.next()
    packet_copy.wait()


def attend(args, dp_size):
    query, keys, w_out, norm_gain, w_in = args[1], args[8], args[10], args[11], args[12]
    col_width = w_out.shape[1]
    tok_rows, head_local, head_dim = query.shape
    cache_len = keys.shape[2]
    width = head_local * head_dim + col_width + 2 * LANES
    copies = 2 if tok_rows % 2 == 0 else tok_rows
    return pl.pallas_call(
        attend_kernel,
        out_shape=(
            pltpu.HBM((dp_size, tok_rows, width), jnp.bfloat16),
            pltpu.VMEM(w_out.shape, w_out.dtype),
            pltpu.VMEM(norm_gain.shape, norm_gain.dtype),
            pltpu.VMEM((w_in.shape[2], in_cut_of(w_in)), w_in.dtype),
        ),
        in_specs=[pl.BlockSpec(memory_space=pl.ANY)] * len(args),
        out_specs=(pl.BlockSpec(memory_space=pl.ANY),)
        + (pl.BlockSpec(memory_space=pltpu.VMEM),) * 3,
        scratch_shapes=[pltpu.VMEM((dp_size, tok_rows, width), jnp.bfloat16)]
        + [pltpu.VMEM(a.shape, a.dtype) for a in args[:10]]
        + [
            pltpu.VMEM((tok_rows, head_local, cache_len), jnp.float32),
            pltpu.SemaphoreType.DMA((10,)),
            pltpu.SemaphoreType.DMA((2 * copies + 2,)),
        ],
        compiler_params=pltpu.CompilerParams(vmem_limit_bytes=58 * MIB),
        cost_estimate=pl.CostEstimate(
            flops=4 * tok_rows * head_local * cache_len * head_dim,
            bytes_accessed=4 * keys.size + 2 * w_out.size,
            transcendentals=tok_rows * head_local * cache_len,
        ),
        name="attend",
    )(*[in_hbm(a) for a in args])


def places_of(ids, tok_rows):
    lane = lax.broadcasted_iota(jnp.int32, (1, LANES), 1)
    places = []
    for j in range(TOP):
        place = jnp.zeros((1, LANES), jnp.int32)
        for back in range(1, tok_rows):
            same = jnp.zeros((1, LANES), jnp.bool_)
            for i in range(TOP):
                same = same | (ids[j] == pltpu.roll(ids[i], back, 1))
            place = place + jnp.where(same & (lane % tok_rows >= back), 1, 0)
        places.append(place)
    return places


def project_kernel(came, w_out, norm_gain, packet, factors, rows):
    dp_size, tok_rows, width = came.shape
    depth, col_width = w_out.shape
    batch = dp_size * tok_rows
    slot_rows = dp_size * MOST
    blocks = slot_rows // ROWS
    experts_at = depth + col_width
    ratio = norm_gain.shape[1] // col_width
    dp_at = lax.axis_index("dp")
    head_at = lax.axis_index("y") * CORES + lax.axis_index("core")
    group_count = dp_size // EXPERTS
    routing = jnp.zeros((tok_rows, 2 * LANES), jnp.float32)
    for d in range(dp_size):
        each = came[d].astype(jnp.float32)
        rows[d * tok_rows : (d + 1) * tok_rows] = each[:, :experts_at]
        routing = routing + each[:, experts_at:]
    ids = [routing[j : j + 1, :LANES].astype(jnp.int32) for j in range(TOP)]
    gates = [
        routing[TOP + j : TOP + j + 1, :LANES]
        + (routing[j : j + 1, LANES:] + routing[TOP + j : TOP + j + 1, LANES:])
        for j in range(TOP)
    ]
    lane = lax.broadcasted_iota(jnp.int32, (1, LANES), 1)
    places = places_of(ids, tok_rows)

    def takes(expert, place, owner):
        hits = []
        for j in range(TOP):
            hit = (owner == lane // tok_rows) & (expert == ids[j]) & (place == places[j])
            hits.append(hit)
        return hits

    row = lax.broadcasted_iota(jnp.int32, (EXPERTS * slot_rows, LANES), 0)
    hits = takes(row // slot_rows, row % MOST, row % slot_rows // MOST)
    picks = jnp.where(hits[0] | hits[1], 1.0, 0.0)[:, :batch].astype(jnp.bfloat16)
    partial = (
        jnp.dot(
            rows[:, :depth].astype(jnp.bfloat16), w_out[...], preferred_element_type=jnp.float32
        )
        + rows[:, depth:]
    ).astype(jnp.bfloat16)
    picked = jnp.dot(picks, partial, preferred_element_type=jnp.float32).astype(jnp.bfloat16)

    gain = jnp.zeros((1, col_width), jnp.float32)
    for r in range(ratio):
        gain = jnp.where(
            dp_at % ratio == r, norm_gain[:, r * col_width : (r + 1) * col_width], gain
        )
    gain = jnp.where(dp_at // ratio == head_at, gain, 0.0)
    high = gain.astype(jnp.bfloat16).astype(jnp.float32)
    gains = [
        part[:, i * LANES : (i + 1) * LANES]
        for part in (high, gain - high)
        for i in range(col_width // LANES)
    ]
    gains = gains + [jnp.zeros((1, LANES), jnp.float32)] * (ROWS - len(gains))
    gains = jnp.concatenate(gains, axis=0).astype(jnp.bfloat16)
    copies = packet.shape[0] // EXPERTS
    for e in range(EXPERTS):
        for i in range(copies):
            to = e * copies + i
            for k in range(blocks):
                first = e * slot_rows + k * ROWS
                packet[to, :, k * col_width : (k + 1) * col_width] = picked[first : first + ROWS]
            packet[to, :, blocks * col_width :] = gains

    row = lax.broadcasted_iota(jnp.int32, (slot_rows, LANES), 0)
    hits = takes(dp_at // group_count, row % MOST, row // MOST)
    weight = sum(jnp.where(hits[j], gates[j], 0.0) for j in range(TOP))
    factors[0] = jnp.broadcast_to(jnp.sum(weight, axis=1, keepdims=True), (slot_rows, LANES))
    first = (head_at == 0) & (dp_at % group_count == 0)
    factors[1] = jnp.full((slot_rows, LANES), jnp.where(first, 1.0 / TOP, 0.0))


def project(came, w_out, norm_gain, y_size):
    dp_size, tok_rows = came.shape[:2]
    depth, col_width = w_out.shape
    slot_rows = dp_size * MOST
    vmem = pl.BlockSpec(memory_space=pltpu.VMEM)
    return pl.pallas_call(
        project_kernel,
        out_shape=(
            jax.ShapeDtypeStruct(
                (dp_size * y_size, ROWS, slot_rows // ROWS * col_width + LANES), jnp.bfloat16
            ),
            jax.ShapeDtypeStruct((2, slot_rows, LANES), jnp.float32),
        ),
        in_specs=[vmem] * 3,
        out_specs=(vmem, vmem),
        scratch_shapes=[pltpu.VMEM((dp_size * tok_rows, depth + col_width), jnp.float32)],
        compiler_params=pltpu.CompilerParams(vmem_limit_bytes=58 * MIB),
        cost_estimate=pl.CostEstimate(
            flops=2 * dp_size * tok_rows * depth * col_width,
            bytes_accessed=2 * depth * col_width,
            transcendentals=0,
        ),
        name="project",
    )(in_vmem(came), in_vmem(w_out), in_vmem(norm_gain))


def early_kernel(arrived, w_in, early, sems):
    copies = [
        pltpu.make_async_copy(cut_at(w_in, 1 + i, early.shape[2]), early.at[i], sems.at[i])
        for i in range(early.shape[0])
    ]
    for copy in copies:
        copy.start()
    for copy in copies:
        copy.wait()


def load_early(arrived, w_in):
    count = min(EARLY, 2 * (w_in.shape[3] // in_cut_of(w_in))) - 1
    shape = (count, w_in.shape[2], in_cut_of(w_in))
    hbm = pl.BlockSpec(memory_space=pl.ANY)
    return pl.pallas_call(
        early_kernel,
        out_shape=pltpu.VMEM(shape, w_in.dtype),
        in_specs=[hbm, hbm],
        out_specs=pl.BlockSpec(memory_space=pltpu.VMEM),
        scratch_shapes=[pltpu.SemaphoreType.DMA((count,))],
        compiler_params=pltpu.CompilerParams(vmem_limit_bytes=1 * MIB),
        cost_estimate=pl.CostEstimate(
            flops=32 * shape[0] * shape[1] * shape[2],
            bytes_accessed=2 * shape[0] * shape[1] * shape[2],
            transcendentals=0,
        ),
        name="load_early",
    )(arrived, in_hbm(w_in))


def expert_kernel(
    arrived, swapped, factors, first_in, early_in, w_in, w_down, out, ins, downs, total, x,
    normed, hidden, in_sems, down_sems,
):
    slot_rows, features = x.shape
    in_cut = ins.shape[2]
    held = 1 + early_in.shape[0]
    in_count = hidden.shape[1] // in_cut
    down_count, down_cut = downs.shape[:2]
    copies = [
        pltpu.make_async_copy(cut_at(w_in, held + i, in_cut), ins.at[i], in_sems.at[i])
        for i in range(2 * in_count - held)
    ]
    copies += [
        pltpu.make_async_copy(
            w_down.at[0, pl.ds(j * down_cut, down_cut)], downs.at[j], down_sems.at[j]
        )
        for j in range(down_count)
    ]
    stream = Stream(copies, AHEAD)
    most, feat_width = out.shape[1:]
    heads = features // feat_width
    y_size = heads // CORES
    dp_size = arrived.shape[0] // y_size
    col_width = features // dp_size
    blocks = slot_rows // ROWS
    square = jnp.zeros((slot_rows, 1), jnp.float32)
    gain = []
    for d in range(dp_size):
        piece = jnp.zeros(arrived.shape[1:], jnp.float32)
        for y in range(y_size):
            at = d * y_size + y
            piece = piece + arrived[at].astype(jnp.float32)
            piece = piece + swapped[at].astype(jnp.float32)
        slots = jnp.concatenate(
            [piece[:, k * col_width : (k + 1) * col_width] for k in range(blocks)], axis=0
        )
        square = square + jnp.sum(slots * slots, axis=1, keepdims=True)
        x[:, d * col_width : (d + 1) * col_width] = slots
        terms = piece[:, blocks * col_width :]
        count = col_width // LANES
        for i in range(count):
            gain.append(terms[i : i + 1] + terms[count + i : count + i + 1])
    scale = lax.rsqrt(square * (1.0 / features) + EPSILON)
    for i in range(features // LANES):
        cut = slice(i * LANES, (i + 1) * LANES)
        normed[:, cut] = (x[:, cut] * scale * gain[i]).astype(jnp.bfloat16)
    for j in range(in_count):
        acts = []
        for i in range(2):
            at = 2 * j + i
            if at == 0:
                cut = first_in[...]
            elif at < held:
                cut = early_in[at - 1]
            else:
                stream.next()
                cut = ins[at - held]
            acts.append(jnp.dot(normed[...], cut, preferred_element_type=jnp.float32))
        hidden[:, j * in_cut : (j + 1) * in_cut] = (jax.nn.silu(acts[0]) * acts[1]).astype(
            jnp.bfloat16
        )
    weight, part = factors[0, :, 0:1], factors[1, :, 0:1]
    last = down_count - 1
    if last == 0:
        total[...] = jnp.zeros_like(total)
    for j in range(last):
        stream.next()
        share = jnp.dot(
            hidden[:, j * down_cut : (j + 1) * down_cut],
            downs[j],
            preferred_element_type=jnp.float32,
        )
        total[...] = share if j == 0 else total[...] + share
    for h in range(heads):
        cut = slice(h * feat_width, (h + 1) * feat_width)
        if h == 0:
            stream.next()
        share = jnp.dot(
            hidden[:, last * down_cut :], downs[last, :, cut], preferred_element_type=jnp.float32
        )
        given = weight * (total[:, cut] + share) + part * x[:, cut]
        for o in range(slot_rows // most):
            out[o * heads + h] = given[o * most : (o + 1) * most].astype(jnp.bfloat16)


def experts(arrived, swapped, factors, first_in, early_in, w_in, w_down, dp_size, feat_width):
    features, width = w_in.shape[2:]
    slot_rows = factors.shape[1]
    in_cut = in_cut_of(w_in)
    left = 2 * (width // in_cut) - 1 - early_in.shape[0]
    vmem, hbm = pl.BlockSpec(memory_space=pltpu.VMEM), pl.BlockSpec(memory_space=pl.ANY)
    return pl.pallas_call(
        expert_kernel,
        out_shape=jax.ShapeDtypeStruct(
            (dp_size * (features // feat_width), MOST, feat_width), jnp.bfloat16
        ),
        in_specs=[vmem] * 5 + [hbm] * 2,
        out_specs=vmem,
        scratch_shapes=[
            pltpu.VMEM((max(left, 1), features, in_cut), jnp.bfloat16),
            pltpu.VMEM((width // in_cut, in_cut, features), jnp.bfloat16),
            pltpu.VMEM((slot_rows, features), jnp.float32),
            pltpu.VMEM((slot_rows, features), jnp.float32),
            pltpu.VMEM((slot_rows, features), jnp.bfloat16),
            pltpu.VMEM((slot_rows, width), jnp.bfloat16),
            pltpu.SemaphoreType.DMA((max(left, 1),)),
            pltpu.SemaphoreType.DMA((width // in_cut,)),
        ],
        compiler_params=pltpu.CompilerParams(vmem_limit_bytes=48 * MIB),
        cost_estimate=pl.CostEstimate(
            flops=6 * slot_rows * features * width,
            bytes_accessed=6 * features * width,
            transcendentals=slot_rows * width,
        ),
        name="experts",
    )(
        in_vmem(arrived),
        in_vmem(swapped),
        in_vmem(factors),
        in_vmem(first_in),
        in_vmem(early_in),
        in_hbm(w_in),
        in_hbm(w_down),
    )


def combine_kernel(back, ids_at, out, rows):
    sources, most, feat_width = back.shape
    tok_rows = out.shape[0]
    pad = jnp.full((TOP, LANES - tok_rows), -1, jnp.int32)
    named = jnp.concatenate([ids_at[...], pad], axis=1)
    ids = [named[j : j + 1] for j in range(TOP)]
    places = places_of(ids, tok_rows)
    row = lax.broadcasted_iota(jnp.int32, (sources * most, LANES), 0)
    expert, place = row // (sources * most // EXPERTS), row % most
    takes = jnp.zeros(row.shape, jnp.float32)
    for j in range(TOP):
        takes = jnp.where((expert == ids[j]) & (place == places[j]), 1.0, takes)
    takes = jnp.transpose(takes)[:ROWS].astype(jnp.bfloat16)
    for i in range(sources):
        rows[i * most : (i + 1) * most] = back[i].astype(jnp.float32)
    total = jnp.dot(takes, rows[...].astype(jnp.bfloat16), preferred_element_type=jnp.float32)
    out[...] = total[:tok_rows].astype(jnp.bfloat16)


def combine(back, ids):
    sources, most, feat_width = back.shape
    tok_rows = ids.shape[1]
    vmem = pl.BlockSpec(memory_space=pltpu.VMEM)
    return pl.pallas_call(
        combine_kernel,
        out_shape=jax.ShapeDtypeStruct((tok_rows, feat_width), jnp.bfloat16),
        in_specs=[vmem, vmem],
        out_specs=vmem,
        scratch_shapes=[pltpu.VMEM((sources * most, feat_width), jnp.float32)],
        compiler_params=pltpu.CompilerParams(vmem_limit_bytes=16 * MIB),
        cost_estimate=pl.CostEstimate(
            flops=2 * tok_rows * back.size, bytes_accessed=2 * back.size, transcendentals=0
        ),
        name="combine",
    )(back, ids)


def shards(
    residual,
    query,
    fresh_token_keys,
    value_new,
    key_cache,
    value_cache,
    lengths,
    pages,
    w_out,
    norm_gain,
    expert_ids,
    gate_weights,
    w_in,
    w_down,
):
    dp_size, y_size = lax.axis_size("dp"), lax.axis_size("y")
    tok_rows, feat_width = residual.shape

    sent, w_out, norm_gain, first_in = attend(
        (
            lengths.reshape(1, tok_rows),
            query,
            fresh_token_keys,
            value_new,
            pages,
            residual,
            expert_ids.T,
            gate_weights.T,
            key_cache,
            value_cache,
            w_out,
            norm_gain.reshape(1, feat_width),
            w_in,
        ),
        dp_size,
    )
    came = lax.all_to_all(sent, "dp", split_axis=0, concat_axis=0, tiled=True)

    packet, factors = project(came, w_out, norm_gain, y_size)
    arrived = lax.all_to_all(packet, ("dp", "y"), split_axis=0, concat_axis=0, tiled=True)
    swapped = lax.ppermute(arrived, "core", [(i, i ^ 1) for i in range(CORES)])
    early_in = load_early(arrived, w_in)
    given_back = experts(
        arrived, swapped, factors, first_in, early_in, w_in, w_down, dp_size, feat_width
    )

    back = lax.all_to_all(
        given_back, ("dp", "y", "core"), split_axis=0, concat_axis=0, tiled=True
    )
    return combine(back, expert_ids.T)


def solution(mesh):
    dp_size, head_size = mesh.shape["dp"], mesh.shape["head"]
    grid = Mesh(mesh.devices.reshape(dp_size, head_size // CORES, CORES), ("dp", "y", "core"))
    head = ("y", "core")
    in_specs = (
        P("dp", head),
        P("dp", head, None),
        P("dp", head, None),
        P("dp", head, None),
        P("dp", head, None, None),
        P("dp", head, None, None),
        P("dp"),
        P("dp", head, None),
        P(head, "dp"),
        P(head),
        P("dp", None),
        P("dp", None),
        P("dp", None, None, head),
        P("dp", head, None),
    )
    return jax.shard_map(
        shards, mesh=grid, in_specs=in_specs, out_specs=P("dp", head), check_vma=False
    )
```
